32 devices in a mesh: row: 8 (over z, core), col: 4 (over y, x).
Axes of the slice: x: 2, y: 2, z: 4, core: 2. Of those that a mesh axis runs over, the one named last changes fastest.
Arguments:
- psi: bfloat16 [1024, 4096], P(('row', 'col')), may hold values from -6 to 6
- hpsi: bfloat16 [1024, 4096], P(('row', 'col')), may hold values from -0.1875 to 0.1875
- eigvec: bfloat16 [4, 8, 128, 8, 4, 128], P(None, 'row', None, None, 'col'), may hold values from -0.09375 to 0.09375
Outputs:
- correlation_tiles: float32 [4, 8, 128, 8, 4, 128], P(None, 'row', None, None, 'col')
- updated_tiles: float32 [4, 8, 128, 8, 4, 128], P(None, 'row', None, None, 'col')
- diag_part: float32 [16], replicated
- offdiag_part: float32 [16], replicated
- rotated: bfloat16 [1024, 8, 4, 128], P('row', None, 'col')
The draws below stay inside these ranges and needn't reach their ends.
All inputs are finite; a program needn't handle non-finite values.
Results may differ from the reference program's by a relative error of at most 0.001.
Values may be sent and summed in bfloat16 or wider, within the bound.
A program may use at most 128 MiB of HBM per device.

```python
import jax
import jax.numpy as jnp
from jax import lax

NB = 4096
TB = 128
PB = 16
NG = 1024
KR = 4
KC = 8
N_ROW = 8
N_COL = 4


def block_levels(key, shape, pieces, least, largest):
    def one(position, shards_of):
        heights = jax.random.uniform(jax.random.fold_in(jax.random.fold_in(key, 6), position), (shards_of,), jnp.float32, least / len(pieces), largest / len(pieces))
        return jnp.repeat(jnp.exp(heights), shape[position] // shards_of).reshape((-1,) + (1,) * (len(shape) - position - 1))

    loudness = one(*pieces[0])
    for cut in pieces[1:]:
        loudness = loudness * one(*cut)
    return loudness


def centred(rng, dims, spread, most, pieces=(), held_as=jnp.bfloat16):
    array = jax.random.normal(rng, dims, jnp.float32) * spread
    if len(pieces) > 0:
        array = block_levels(rng, dims, pieces, -0.22, 0.18) * array
    return jnp.clip(array, min=-most, max=most).astype(held_as)


def setup_inputs(seed: int = 0) -> dict:
    splits = jax.random.split(jax.random.key(seed), 4)
    psi = centred(splits[0], (NG, NB), 1.0, 6.0, ((0, 32),))
    hpsi = centred(splits[1], (NG, NB), NG ** -0.5, 0.1875, ((0, 32),))
    eigvec = centred(splits[2], (KR, N_ROW, TB, KC, N_COL, TB), NB ** -0.5, 0.09375, ((1, 8), (4, 4)))
    return dict(psi=psi, hpsi=hpsi, eigvec=eigvec)


def reference(psi, hpsi, eigvec):
    highest = lax.Precision.HIGHEST
    mixed = jnp.dot(psi.T, hpsi, preferred_element_type=jnp.float32)
    reduced = 0.5 * (mixed + mixed.T)
    correlation = jnp.dot(psi.T, psi, preferred_element_type=jnp.float32) / float(NG)
    panel = reduced[:, :PB]
    positions = jnp.arange(NB)
    vecs = jnp.zeros((NB, PB), jnp.float32)
    images = jnp.zeros((NB, PB), jnp.float32)
    diag_list = []
    off_list = []
    for step in range(PB):
        column = panel[:, step] - jnp.dot(vecs, images[step], precision=highest) - jnp.dot(images, vecs[step], precision=highest)
        pivot = column[step + 1]
        below = positions > step + 1
        tail = jnp.sum(jnp.where(below, column * column, 0.0))
        length = jnp.sqrt(pivot * pivot + tail)
        beta = jnp.where(pivot >= 0.0, -length, length)
        tau = (beta - pivot) / beta
        vector = jnp.where(positions == step + 1, 1.0, jnp.where(below, column / (pivot - beta), 0.0))
        image = jnp.dot(reduced, vector, precision=highest)
        image = image - jnp.dot(vecs, jnp.dot(vector, images, precision=highest), precision=highest)
        image = image - jnp.dot(images, jnp.dot(vector, vecs, precision=highest), precision=highest)
        image = tau * image
        image = image - 0.5 * tau * jnp.dot(image, vector, precision=highest) * vector
        vecs = vecs.at[:, step].set(vector)
        images = images.at[:, step].set(image)
        diag_list.append(column[step])
        off_list.append(beta)
    updated = reduced - jnp.dot(vecs, images.T, precision=highest) - jnp.dot(images, vecs.T, precision=highest)
    rotation = eigvec.reshape(NB, NB)
    rotated = jnp.dot(psi, rotation, preferred_element_type=jnp.float32).astype(jnp.bfloat16)
    tile_shape = (KR, N_ROW, TB, KC, N_COL, TB)
    return (correlation.reshape(tile_shape), updated.reshape(tile_shape), jnp.stack(diag_list).astype(jnp.float32), jnp.stack(off_list).astype(jnp.float32), rotated.reshape(NG, KC, N_COL, TB))
```

```python
import functools

import jax
import jax.numpy as jnp
from jax import lax
from jax.experimental import pallas as pl
from jax.experimental.pallas import tpu as pltpu
from jax.sharding import PartitionSpec as P

PB = 16
LEAD = 32
F32 = jnp.float32
BF16 = jnp.bfloat16
MESH = pl.DeviceIdType.MESH


def inner(left, right):
    return lax.dot_general(
        left, right, (((0,), (0,)), ((), ())), preferred_element_type=F32
    )


def remote(source, target, send, recv, device):
    return pltpu.make_async_remote_copy(
        src_ref=source, dst_ref=target, send_sem=send, recv_sem=recv,
        device_id=device, device_id_type=MESH,
    )


def enter(devices):
    barrier = pltpu.get_barrier_semaphore()
    for device in devices:
        pl.semaphore_signal(barrier, inc=1, device_id=device, device_id_type=MESH)
    pl.semaphore_wait(barrier, len(devices))


def spread_kernel(
    sizes, psi, hpsi, col_all, row_all, lead_all,
    stage, s1_send, s1_recv, up_send, up_recv, down_send, down_recv,
    sib_send, sib_recv, leadz_send, leadz_recv, leadp_send, leadp_recv,
    row_send, row_recv, own_sem,
):
    row_count, col_count, row_tiles, col_tiles, tile = sizes
    levels = row_count // 2
    half = row_tiles * tile
    r = lax.axis_index("row")
    c = lax.axis_index("col")
    z = lax.div(r, 2)
    k = lax.rem(r, 2)
    sib = (r + 1 - 2 * k, c)

    def turn(d):
        return lax.rem(c + d, col_count)

    for target in range(col_count):
        for a, source in enumerate((psi, hpsi)):
            for parity in range(2):
                for t in range(row_tiles):
                    j = target + col_count * parity + row_count * t
                    at = (parity * row_tiles + t) * tile
                    stage[target, a, :, at : at + tile] = source[:, j * tile : (j + 1) * tile]
    col_all[:, z, k, c] = stage[c]

    peers = [(r, turn(d)) for d in range(1, col_count)]
    peers += [(lax.rem(r + 2 * d, row_count), c) for d in range(1, levels)]
    peers += [(sib[0], turn(d)) for d in range(col_count)]
    enter(peers)

    def first(d):
        return remote(
            stage.at[turn(d)], col_all.at[:, z, k, c], s1_send.at[d], s1_recv.at[d], (r, turn(d))
        )

    def first_in(d):
        place = col_all.at[:, z, k, turn(col_count - d)]
        return remote(place, place, s1_send.at[d], s1_recv.at[d], (r, turn(d)))

    def up(o, d):
        place = col_all.at[:, z - o, k, turn(d)]
        return remote(place, place, up_send.at[o, d], up_recv.at[o, d], (r + 2, c))

    def up_in(o, d):
        place = col_all.at[:, z - 1 - o, k, turn(d)]
        return remote(place, place, up_send.at[o, d], up_recv.at[o, d], (r + 2, c))

    def down(o, d):
        place = col_all.at[:, z + o, k, turn(d)]
        return remote(place, place, down_send.at[o, d], down_recv.at[o, d], (r - 2, c))

    def down_in(o, d):
        place = col_all.at[:, z + 1 + o, k, turn(d)]
        return remote(place, place, down_send.at[o, d], down_recv.at[o, d], (r - 2, c))

    def across(level, d):
        place = col_all.at[:, level, k, turn(d)]
        return remote(place, place, sib_send.at[level, d], sib_recv.at[level, d], sib)

    def across_in(level, d):
        place = col_all.at[:, level, 1 - k, turn(d)]
        return remote(place, place, sib_send.at[level, d], sib_recv.at[level, d], sib)

    not_top = z < levels - 1
    not_bottom = z > 0

    def launch(d):
        @pl.when(not_top)
        def _():
            up(0, d).start()

        @pl.when(not_bottom)
        def _():
            down(0, d).start()

        across(z, d).start()

    for d in range(1, col_count):
        first(d).start()
    launch(0)
    order = [col_count - d for d in range(1, col_count)]
    for d in range(1, col_count):
        first_in(d).wait_recv()
        launch(order[d - 1])

    def lead_z(d):
        place = lead_all.at[z, k]
        return remote(
            place, place, leadz_send.at[d], leadz_recv.at[d], (lax.rem(r + 2 * d, row_count), c)
        )

    def lead_z_in(d):
        place = lead_all.at[lax.rem(z + levels - d, levels), k]
        return remote(place, place, leadz_send.at[d], leadz_recv.at[d], (r, c))

    def flat(q):
        return (2 * z + q // col_count, q % col_count)

    def lead_plane(d, q):
        level = lax.rem(z + levels - d, levels)
        place = lead_all.at[level, k]
        return remote(place, place, leadp_send.at[d, q], leadp_recv.at[level, k], flat(q))

    def lead_plane_in(level, kk):
        place = lead_all.at[level, kk]
        return remote(place, place, leadp_send.at[0, 0], leadp_recv.at[level, kk], (r, c))

    def each_peer(action):
        for q in range(2 * col_count):
            @pl.when(k * col_count != q)
            def _():
                action(q)

    @pl.when(c == 0)
    def _():
        for a in range(2):
            block = col_all[a, z, k, :, :, 0:tile].astype(F32)
            block = block.reshape(block.shape[0] * block.shape[1], tile)
            lead_all[z, k, a] = jnp.transpose(block)[0:LEAD].astype(BF16)
        for d in range(1, levels):
            lead_z(d).start()
        each_peer(lambda q: lead_plane(0, q).start())

    source_c = lax.rem(r, col_count)
    source_half = lax.div(r, col_count)
    lane0 = pl.multiple_of(source_half * half, half)
    partner = c + 1 - 2 * lax.rem(c, 2)
    is_source = c == source_c
    is_relay = jnp.logical_and(c != source_c, lax.rem(c, 2) == lax.rem(source_c, 2))

    def row_own(level, kk):
        return pltpu.make_async_copy(
            col_all.at[:, level, kk, :, :, pl.ds(lane0, half)],
            row_all.at[:, level, kk], own_sem.at[level, kk],
        )

    def row_out(level, kk, i):
        device = (r, partner) if i == 0 else (r, lax.rem(c + 2 * i, col_count))
        return remote(
            col_all.at[:, level, kk, :, :, pl.ds(lane0, half)],
            row_all.at[:, level, kk],
            row_send.at[level, kk, i], row_recv.at[level, kk], device,
        )

    def row_relay(level, kk):
        place = row_all.at[:, level, kk]
        return remote(
            place, place, row_send.at[level, kk, 0], row_recv.at[level, kk], (r, partner)
        )

    fan = col_count // 2

    def row_launch(level):
        @pl.when(is_source)
        def _():
            for kk in range(2):
                for i in range(fan):
                    row_out(level, kk, i).start()
                row_own(level, kk).start()

    def row_finish(level):
        @pl.when(is_relay)
        def _():
            for kk in range(2):
                row_relay(level, kk).wait_recv()
                row_relay(level, kk).start()

    def settle(level):
        for d in range(col_count):
            across_in(level, d).wait_recv()
        row_launch(level)

    settle(z)
    for o in range(levels - 1):
        below = z - 1 - o >= 0
        above = z + 1 + o <= levels - 1
        for d in [0] + order:
            @pl.when(below)
            def _():
                up_in(o, d).wait_recv()

                @pl.when(not_top)
                def _():
                    up(o + 1, d).start()

                across(z - 1 - o, d).start()

            @pl.when(above)
            def _():
                down_in(o, d).wait_recv()

                @pl.when(not_bottom)
                def _():
                    down(o + 1, d).start()

                across(z + 1 + o, d).start()

        if o == 0:
            row_finish(z)

            @pl.when(c == 0)
            def _():
                for d in range(1, levels):
                    lead_z_in(d).wait_recv()
                    each_peer(lambda q: lead_plane(d, q).start())
        else:
            @pl.when(z - o >= 0)
            def _():
                row_finish(z - o)

            @pl.when(z + o <= levels - 1)
            def _():
                row_finish(z + o)

        @pl.when(below)
        def _():
            settle(z - 1 - o)

        @pl.when(above)
        def _():
            settle(z + 1 + o)

    @pl.when(z - (levels - 1) >= 0)
    def _():
        row_finish(z - (levels - 1))

    @pl.when(z + levels - 1 <= levels - 1)
    def _():
        row_finish(z + levels - 1)

    for level in range(levels):
        for kk in range(2):
            @pl.when(is_source)
            def _():
                for i in range(fan):
                    row_out(level, kk, i).wait_send()
                row_own(level, kk).wait()

            @pl.when(is_relay)
            def _():
                row_relay(level, kk).wait_send()

            @pl.when(jnp.logical_not(jnp.logical_or(is_source, is_relay)))
            def _():
                row_relay(level, kk).wait_recv()

            @pl.when(jnp.logical_or(c != 0, k != kk))
            def _():
                lead_plane_in(level, kk).wait_recv()

    @pl.when(c == 0)
    def _():
        for d in range(1, levels):
            lead_z(d).wait_send()
        for d in range(levels):
            each_peer(lambda q: lead_plane(d, q).wait_send())

    for d in range(1, col_count):
        first(d).wait_send()
    for o in range(levels):
        for d in range(col_count):
            @pl.when(jnp.logical_and(not_top, z - o >= 0))
            def _():
                up(o, d).wait_send()

            @pl.when(jnp.logical_and(not_bottom, z + o <= levels - 1))
            def _():
                down(o, d).wait_send()

    for level in range(levels):
        for d in range(col_count):
            across(level, d).wait_send()


def spread(psi, hpsi, sizes):
    row_count, col_count, row_tiles, col_tiles, tile = sizes
    g_rows = psi.shape[0]
    levels = row_count // 2
    whole = pl.BlockSpec(memory_space=pltpu.VMEM)
    dma = pltpu.SemaphoreType.DMA
    return pl.pallas_call(
        functools.partial(spread_kernel, sizes),
        out_shape=(
            jax.ShapeDtypeStruct((2, levels, 2, col_count, g_rows, col_tiles * tile), BF16),
            jax.ShapeDtypeStruct((2, levels, 2, col_count, g_rows, row_tiles * tile), BF16),
            jax.ShapeDtypeStruct((levels, 2, 2, LEAD, col_count * g_rows), BF16),
        ),
        in_specs=[whole, whole],
        out_specs=(whole, whole, whole),
        scratch_shapes=[
            pltpu.VMEM((col_count, 2, g_rows, col_tiles * tile), BF16),
            dma((col_count,)), dma((col_count,)),
            dma((levels, col_count)), dma((levels, col_count)),
            dma((levels, col_count)), dma((levels, col_count)),
            dma((levels, col_count)), dma((levels, col_count)),
            dma((levels,)), dma((levels,)),
            dma((levels, 2 * col_count)), dma((levels, 2)),
            dma((levels, 2, col_count // 2)), dma((levels, 2)),
            dma((levels, 2)),
        ],
        compiler_params=pltpu.CompilerParams(
            collective_id=1, has_side_effects=True, vmem_limit_bytes=40 * 1024 * 1024
        ),
        cost_estimate=pl.CostEstimate(
            flops=100_000_000, bytes_accessed=8_000_000, transcendentals=0
        ),
        name="spread",
    )(psi, hpsi)


def lanes_sum(array):
    return jnp.sum(array, axis=1, keepdims=True)


def rows_sum(array):
    return jnp.sum(array, axis=0, keepdims=True)


def parts_of(array):
    high = array.astype(BF16).astype(F32)
    rest = array - high
    middle = rest.astype(BF16).astype(F32)
    return high, middle, rest - middle


def panel_kernel(
    sizes, col_all, lead_all, left, right, diagonal, offdiag,
    natural, turned, panel, vw, message, outgoing, msg_send, msg_recv, end_send, end_recv,
):
    row_count, col_count, row_tiles, col_tiles, tile = sizes
    levels = row_count // 2
    half = row_tiles * tile
    group = 2 * col_count
    r = lax.axis_index("row")
    c = lax.axis_index("col")
    z = lax.div(r, 2)
    k = lax.rem(r, 2)
    part = k * col_count + c
    blocks = levels * 2
    gvecs = natural.shape[1]
    deep = gvecs // blocks

    def peer(d):
        q = lax.rem(part + d, group)
        return (2 * z + lax.div(q, col_count), lax.rem(q, col_count))

    message[...] = jnp.zeros_like(message)
    enter([peer(d) for d in range(1, group)])

    for a in range(2):
        for level in range(levels):
            for kk in range(2):
                at = (level * 2 + kk) * deep
                own = col_all[a, level, kk, :, :, pl.ds(pl.multiple_of(k * half, half), half)]
                own = own.reshape(deep, half)
                natural[a, at : at + deep, 0:half] = own
                turned[a, :, at : at + deep] = jnp.transpose(own.astype(F32)).astype(BF16)
                lead = lead_all[level, kk, a].astype(F32)
                lead = jnp.concatenate(
                    [lead, jnp.zeros((tile - LEAD, deep), F32)], axis=0
                )
                natural[a, at : at + deep, half : half + tile] = jnp.transpose(lead).astype(BF16)
    start = jnp.zeros((LEAD, half + tile), F32)
    for level in range(levels):
        for kk in range(2):
            at = (level * 2 + kk) * deep
            for a in range(2):
                start = start + jnp.dot(
                    lead_all[level, kk, a], natural[1 - a, at : at + deep, :],
                    preferred_element_type=F32,
                )
    panel[...] = 0.5 * start
    vw[...] = jnp.zeros_like(vw)
    diagonal[...] = jnp.zeros_like(diagonal)
    offdiag[...] = jnp.zeros_like(offdiag)

    wide = half + tile
    lane = lax.broadcasted_iota(jnp.int32, (1, wide), 1)
    own_tile = lax.div(lane, tile)
    inside = lane - own_tile * tile
    pos = jnp.where(lane < half, (own_tile * row_count + part) * tile + inside, lane - half)
    lane1 = lax.broadcasted_iota(jnp.int32, (1, tile), 1)
    lane2 = lax.broadcasted_iota(jnp.int32, (2 * PB, tile), 1)
    sub2 = lax.broadcasted_iota(jnp.int32, (2 * PB, tile), 0)
    group_row = lax.broadcasted_iota(jnp.int32, (group, 2 * gvecs + tile), 0)
    sub8 = lax.broadcasted_iota(jnp.int32, (8, half), 0)

    def swap(column):
        return jnp.concatenate([column[PB:], column[:PB]], axis=0)

    def send(slot, d):
        return remote(
            outgoing.at[slot, pl.ds(0, 1)], message.at[slot, pl.ds(part, 1)], msg_send.at[slot, d], msg_recv.at[slot, d], peer(d),
        )

    @pl.loop(0, PB)
    def _(step):
        slot = lax.rem(step, 2)
        both = vw[...]
        lead_vw = both[:, half:]
        head = lanes_sum(jnp.where(lane2 == step, lead_vw, 0.0))
        column = panel[pl.ds(step, 1), :] - rows_sum(both * swap(head))
        below = pos > step + 1
        masked = jnp.where(below, column, 0.0)[:, :half]
        high, middle, low = parts_of(masked)
        stacked = jnp.where(
            sub8 == 0, high, jnp.where(sub8 == 1, middle, jnp.where(sub8 == 2, low, 0.0))
        ).astype(BF16)
        images = []
        for a in range(2):
            image = rows_sum(jnp.dot(stacked, turned[a], preferred_element_type=F32))
            outgoing[slot, 0:1, a * gvecs : (a + 1) * gvecs] = image
            images.append(image)
        onto = lanes_sum(both[:, :half] * masked)
        tail = lanes_sum(masked * masked)
        small = rows_sum(jnp.where(lane2 == sub2, onto, 0.0)) + jnp.where(
            lane1 == 2 * PB, tail, 0.0
        )
        outgoing[slot, 0:1, 2 * gvecs : 2 * gvecs + tile] = small
        mine = jnp.concatenate(images + [small], axis=1)
        sent = [send(slot, d) for d in range(1, group)]
        for copy in sent:
            copy.start()
        lead_column = column[:, half:]
        pivot = lanes_sum(jnp.where(lane1 == step + 1, lead_column, 0.0))
        here = lanes_sum(jnp.where(lane1 == step, lead_column, 0.0))
        next_row = panel[pl.ds(step + 1, 1), :]
        corner = lanes_sum(jnp.where(lane1 == step + 1, next_row[:, half:], 0.0))
        head_next = lanes_sum(jnp.where(lane2 == step + 1, lead_vw, 0.0))
        for copy in sent:
            copy.wait()
        received = message[slot] + jnp.where(group_row == part, mine, 0.0)
        sums = received[:, : 2 * gvecs]
        pieces = jnp.concatenate(parts_of(sums) + (jnp.zeros_like(sums),), axis=0)
        pieces = pieces.astype(BF16)
        product = rows_sum(
            jnp.dot(pieces[:, :gvecs], natural[1], preferred_element_type=F32)
            + jnp.dot(pieces[:, gvecs:], natural[0], preferred_element_type=F32)
        ) * 0.5
        whole_sum = rows_sum(sums)
        square = lanes_sum(whole_sum[:, :gvecs] * whole_sum[:, gvecs:])
        small = rows_sum(received[:, 2 * gvecs :])
        tail = lanes_sum(jnp.where(lane1 == 2 * PB, small, 0.0))
        onto = lanes_sum(jnp.where(lane2 == sub2, small, 0.0))
        length = jnp.sqrt(pivot * pivot + tail)
        beta = jnp.where(pivot >= 0.0, -length, length)
        tau = (beta - pivot) / beta
        inverse = 1.0 / (pivot - beta)
        vector = jnp.where(
            pos == step + 1, 1.0, jnp.where(below, column * inverse, 0.0)
        )
        onto = onto * inverse + head_next
        image = tau * (product * inverse + next_row - rows_sum(both * swap(onto)))
        edge = lanes_sum(jnp.where(lane1 == step + 1, product[:, half:], 0.0))
        energy = square * inverse * inverse + 2.0 * inverse * edge + corner
        overlap = tau * (energy - 2.0 * rows_sum(onto[:PB] * onto[PB:]))
        image = image - 0.5 * tau * overlap * vector
        vw[pl.ds(step, 1), :] = vector
        vw[pl.ds(PB + step, 1), :] = image
        diagonal[...] = jnp.where(lane1 == step, here, diagonal[...])
        offdiag[...] = jnp.where(lane1 == step, beta, offdiag[...])

    final = vw[:, 0:half]
    right[pl.ds(k, 1)] = final[None]
    across = remote(
        right.at[k], right.at[k], end_send.at[col_count], end_recv.at[1], (r + 1 - 2 * k, c)
    )
    across.start()

    def to_row(j):
        return remote(
            right.at[k], left, end_send.at[j], end_recv.at[0], (part, j)
        )

    mine = jnp.logical_and(part >= 2 * z, part < 2 * z + 2)
    for j in range(col_count):
        @pl.when(jnp.logical_and(mine, jnp.logical_not(jnp.logical_and(part == r, c == j))))
        def _():
            to_row(j).start()

    @pl.when(part == r)
    def _():
        left[...] = final

    @pl.when(part != r)
    def _():
        to_row(0).wait_recv()

    across_in = remote(
        right.at[1 - k], right.at[1 - k], end_send.at[col_count], end_recv.at[1], (r, c)
    )
    across_in.wait_recv()
    across.wait_send()
    for j in range(col_count):
        @pl.when(jnp.logical_and(mine, jnp.logical_not(jnp.logical_and(part == r, c == j))))
        def _():
            to_row(j).wait_send()


def reduce_panel(col_all, lead_all, sizes):
    row_count, col_count, row_tiles, col_tiles, tile = sizes
    half = row_tiles * tile
    gvecs = row_count * col_count * col_all.shape[4]
    group = 2 * col_count
    whole = pl.BlockSpec(memory_space=pltpu.VMEM)
    dma = pltpu.SemaphoreType.DMA
    return pl.pallas_call(
        functools.partial(panel_kernel, sizes),
        out_shape=(
            jax.ShapeDtypeStruct((2 * PB, half), F32),
            jax.ShapeDtypeStruct((2, 2 * PB, half), F32),
            jax.ShapeDtypeStruct((1, tile), F32),
            jax.ShapeDtypeStruct((1, tile), F32),
        ),
        in_specs=[whole, whole],
        out_specs=(whole, whole, whole, whole),
        scratch_shapes=[
            pltpu.VMEM((2, gvecs, half + tile), BF16),
            pltpu.VMEM((2, half, gvecs), BF16),
            pltpu.VMEM((LEAD, half + tile), F32),
            pltpu.VMEM((2 * PB, half + tile), F32),
            pltpu.VMEM((2, group, 2 * gvecs + tile), F32),
            pltpu.VMEM((2, 8, 2 * gvecs + tile), F32),
            dma((2, group)), dma((2, group)),
            dma((col_count + 1,)), dma((2,)),
        ],
        compiler_params=pltpu.CompilerParams(
            collective_id=0, has_side_effects=True, vmem_limit_bytes=40 * 1024 * 1024
        ),
        cost_estimate=pl.CostEstimate(
            flops=400_000_000, bytes_accessed=4_000_000, transcendentals=0
        ),
        name="panel",
    )(col_all, lead_all)


def on_device(psi, hpsi, eigvec):
    highest = lax.Precision.HIGHEST
    row_tiles = eigvec.shape[0]
    tile = eigvec.shape[2]
    col_tiles = eigvec.shape[3]
    row_count = lax.axis_size("row")
    col_count = lax.axis_size("col")
    gvecs = psi.shape[0] * row_count * col_count
    row_width = row_tiles * tile
    col_width = col_tiles * tile
    sizes = (row_count, col_count, row_tiles, col_tiles, tile)
    col_all, row_all, lead_all = spread(psi, hpsi, sizes)
    psi_rows = row_all[0].reshape(gvecs, row_width)
    hpsi_rows = row_all[1].reshape(gvecs, row_width)
    psi_cols = col_all[0].reshape(gvecs, col_width)
    hpsi_cols = col_all[1].reshape(gvecs, col_width)
    reduced = 0.5 * (inner(psi_rows, hpsi_cols) + inner(hpsi_rows, psi_cols))
    correlation = inner(psi_rows, psi_cols) / float(gvecs)
    left, right, diagonal, offdiag = reduce_panel(col_all, lead_all, sizes)
    right = jnp.concatenate([right[:, PB:], right[:, :PB]], axis=1)
    right = jnp.concatenate([right[0], right[1]], axis=1)
    updated = reduced - lax.dot_general(
        left, right, (((0,), (0,)), ((), ())), precision=highest,
        preferred_element_type=F32,
    )
    flat = eigvec.reshape(row_width, col_width)
    rotated = lax.psum_scatter(
        jnp.dot(psi_rows, flat, preferred_element_type=F32),
        "row",
        scatter_dimension=0,
        tiled=True,
    )
    tile_shape = (row_tiles, 1, tile, col_tiles, 1, tile)

    def in_order(matrix):
        matrix = matrix.reshape(row_width, 2, row_tiles, tile)
        return jnp.transpose(matrix, (0, 2, 1, 3)).reshape(tile_shape)

    return (
        in_order(correlation),
        in_order(updated),
        diagonal[0, :PB],
        offdiag[0, :PB],
        rotated.astype(BF16).reshape(rotated.shape[0], col_tiles, 1, tile),
    )


def solution(mesh):
    return jax.shard_map(
        on_device,
        mesh=mesh,
        in_specs=(
            P(("row", "col"), None),
            P(("row", "col"), None),
            P(None, "row", None, None, "col", None),
        ),
        out_specs=(
            P(None, "row", None, None, "col", None),
            P(None, "row", None, None, "col", None),
            P(),
            P(),
            P("row", None, "col", None),
        ),
        check_vma=False,
    )
```

```python
import functools

import jax
import jax.numpy as jnp
from jax import lax
from jax.experimental import pallas as pl
from jax.experimental.pallas import tpu as pltpu
from jax.sharding import PartitionSpec as P

PB = 16
LEAD = 32
F32 = jnp.float32
BF16 = jnp.bfloat16
MESH = pl.DeviceIdType.MESH


def inner(left, right):
    return lax.dot_general(
        left, right, (((0,), (0,)), ((), ())), preferred_element_type=F32
    )


def remote(source, target, send, recv, device):
    return pltpu.make_async_remote_copy(
        src_ref=source, dst_ref=target, send_sem=send, recv_sem=recv,
        device_id=device, device_id_type=MESH,
    )


def enter(devices):
    barrier = pltpu.get_barrier_semaphore()
    for device in devices:
        pl.semaphore_signal(barrier, inc=1, device_id=device, device_id_type=MESH)
    pl.semaphore_wait(barrier, len(devices))


def lanes_sum(array):
    return jnp.sum(array, axis=1, keepdims=True)


def rows_sum(array):
    return jnp.sum(array, axis=0, keepdims=True)


def parts_of(array):
    high = array.astype(BF16).astype(F32)
    rest = array - high
    middle = rest.astype(BF16).astype(F32)
    return high, middle, rest - middle


def step_kernel(
    sizes, psi, hpsi, eig,
    reduced, correlation, left, right, diagonal, offdiag, rotated,
    col_all, row_all, lead_all, stage, natural, turned, panel, vw, message, outgoing,
    keep, give, take, inbox, spun,
    s1_send, s1_recv, up_send, up_recv, down_send, down_recv,
    sib_send, sib_recv, leadz_send, leadz_recv, leadp_send, leadp_recv,
    row_send, row_recv, own_sem, msg_send, msg_recv, end_send, end_recv,
    swap_send, swap_recv, sum_send, sum_recv, spin_sem,
):
    row_count, col_count, row_tiles, col_tiles, tile = sizes
    levels = row_count // 2
    half = row_tiles * tile
    r = lax.axis_index("row")
    c = lax.axis_index("col")
    z = lax.div(r, 2)
    k = lax.rem(r, 2)
    sib = (r + 1 - 2 * k, c)
    group = 2 * col_count
    part = k * col_count + c
    gvecs = natural.shape[1]
    deep = gvecs // row_count

    def peer(d):
        q = lax.rem(part + d, group)
        return (2 * z + lax.div(q, col_count), lax.rem(q, col_count))

    def along(d):
        return (lax.rem(r + 2 * d, row_count), c)

    def turn(d):
        return lax.rem(c + d, col_count)

    for target in range(col_count):
        for a, source in enumerate((psi, hpsi)):
            for parity in range(2):
                for t in range(row_tiles):
                    j = target + col_count * parity + row_count * t
                    at = (parity * row_tiles + t) * tile
                    stage[target, a, :, at : at + tile] = source[:, j * tile : (j + 1) * tile]
    col_all[:, z, k, c] = stage[c]

    message[...] = jnp.zeros_like(message)
    enter([peer(d) for d in range(1, group)] + [along(d) for d in range(1, levels)])

    def first(d):
        return remote(
            stage.at[turn(d)], col_all.at[:, z, k, c], s1_send.at[d], s1_recv.at[d], (r, turn(d))
        )

    def first_in(d):
        place = col_all.at[:, z, k, turn(col_count - d)]
        return remote(place, place, s1_send.at[d], s1_recv.at[d], (r, turn(d)))

    def up(o, d):
        place = col_all.at[:, z - o, k, turn(d)]
        return remote(place, place, up_send.at[o, d], up_recv.at[o, d], (r + 2, c))

    def up_in(o, d):
        place = col_all.at[:, z - 1 - o, k, turn(d)]
        return remote(place, place, up_send.at[o, d], up_recv.at[o, d], (r + 2, c))

    def down(o, d):
        place = col_all.at[:, z + o, k, turn(d)]
        return remote(place, place, down_send.at[o, d], down_recv.at[o, d], (r - 2, c))

    def down_in(o, d):
        place = col_all.at[:, z + 1 + o, k, turn(d)]
        return remote(place, place, down_send.at[o, d], down_recv.at[o, d], (r - 2, c))

    def across(level, d):
        place = col_all.at[:, level, k, turn(d)]
        return remote(place, place, sib_send.at[level, d], sib_recv.at[level, d], sib)

    def across_in(level, d):
        place = col_all.at[:, level, 1 - k, turn(d)]
        return remote(place, place, sib_send.at[level, d], sib_recv.at[level, d], sib)

    not_top = z < levels - 1
    not_bottom = z > 0

    def launch(d):
        @pl.when(not_top)
        def _():
            up(0, d).start()

        @pl.when(not_bottom)
        def _():
            down(0, d).start()

        across(z, d).start()

    for d in range(1, col_count):
        first(d).start()
    launch(0)
    order = [col_count - d for d in range(1, col_count)]
    for d in range(1, col_count):
        first_in(d).wait_recv()
        launch(order[d - 1])

    def lead_z(d):
        place = lead_all.at[z, k]
        return remote(
            place, place, leadz_send.at[d], leadz_recv.at[d], (lax.rem(r + 2 * d, row_count), c)
        )

    def lead_z_in(d):
        place = lead_all.at[lax.rem(z + levels - d, levels), k]
        return remote(place, place, leadz_send.at[d], leadz_recv.at[d], (r, c))

    def flat(q):
        return (2 * z + q // col_count, q % col_count)

    def lead_plane(d, q):
        level = lax.rem(z + levels - d, levels)
        place = lead_all.at[level, k]
        return remote(place, place, leadp_send.at[d, q], leadp_recv.at[level, k], flat(q))

    def lead_plane_in(level, kk):
        place = lead_all.at[level, kk]
        return remote(place, place, leadp_send.at[0, 0], leadp_recv.at[level, kk], (r, c))

    def each_peer(action):
        for q in range(2 * col_count):
            @pl.when(k * col_count != q)
            def _():
                action(q)

    @pl.when(c == 0)
    def _():
        for a in range(2):
            block = col_all[a, z, k, :, :, 0:tile].astype(F32)
            block = block.reshape(block.shape[0] * block.shape[1], tile)
            lead_all[z, k, a] = jnp.transpose(block)[0:LEAD].astype(BF16)
        for d in range(1, levels):
            lead_z(d).start()
        each_peer(lambda q: lead_plane(0, q).start())

    source_c = lax.rem(r, col_count)
    source_half = lax.div(r, col_count)
    lane0 = pl.multiple_of(source_half * half, half)
    partner = c + 1 - 2 * lax.rem(c, 2)
    is_source = c == source_c
    is_relay = jnp.logical_and(c != source_c, lax.rem(c, 2) == lax.rem(source_c, 2))

    def row_own(level, kk):
        return pltpu.make_async_copy(
            col_all.at[:, level, kk, :, :, pl.ds(lane0, half)],
            row_all.at[:, level, kk], own_sem.at[level, kk],
        )

    def row_out(level, kk, i):
        device = (r, partner) if i == 0 else (r, lax.rem(c + 2 * i, col_count))
        return remote(
            col_all.at[:, level, kk, :, :, pl.ds(lane0, half)],
            row_all.at[:, level, kk],
            row_send.at[level, kk, i], row_recv.at[level, kk], device,
        )

    def row_relay(level, kk):
        place = row_all.at[:, level, kk]
        return remote(
            place, place, row_send.at[level, kk, 0], row_recv.at[level, kk], (r, partner)
        )

    fan = col_count // 2

    def row_launch(level):
        @pl.when(is_source)
        def _():
            for kk in range(2):
                for i in range(fan):
                    row_out(level, kk, i).start()
                row_own(level, kk).start()

    def row_finish(level):
        @pl.when(is_relay)
        def _():
            for kk in range(2):
                row_relay(level, kk).wait_recv()
                row_relay(level, kk).start()

    def settle(level):
        for d in range(col_count):
            across_in(level, d).wait_recv()
        row_launch(level)

    def absorb(level):
        for kk in range(2):
            at = pl.multiple_of((level * 2 + kk) * deep, deep)

            @pl.when(jnp.logical_or(c != 0, k != kk))
            def _():
                lead_plane_in(level, kk).wait_recv()

            for a in range(2):
                own = col_all[a, level, kk, :, :, pl.ds(pl.multiple_of(k * half, half), half)]
                own = own.reshape(deep, half)
                natural[a, pl.ds(at, deep), 0:half] = own
                turned[a, :, pl.ds(at, deep)] = jnp.transpose(own.astype(F32)).astype(BF16)
                lead = lead_all[level, kk, a].astype(F32)
                lead = jnp.concatenate(
                    [lead, jnp.zeros((tile - LEAD, deep), F32)], axis=0
                )
                natural[a, pl.ds(at, deep), half : half + tile] = (
                    jnp.transpose(lead).astype(BF16)
                )

    settle(z)
    for o in range(levels - 1):
        below = z - 1 - o >= 0
        above = z + 1 + o <= levels - 1
        for d in [0] + order:
            @pl.when(below)
            def _():
                up_in(o, d).wait_recv()

                @pl.when(not_top)
                def _():
                    up(o + 1, d).start()

                across(z - 1 - o, d).start()

            @pl.when(above)
            def _():
                down_in(o, d).wait_recv()

                @pl.when(not_bottom)
                def _():
                    down(o + 1, d).start()

                across(z + 1 + o, d).start()

        if o == 0:
            @pl.when(c == 0)
            def _():
                for d in range(1, levels):
                    lead_z_in(d).wait_recv()
                    each_peer(lambda q: lead_plane(d, q).start())

            row_finish(z)
            absorb(z)
        else:
            @pl.when(z - o >= 0)
            def _():
                row_finish(z - o)
                absorb(z - o)

            @pl.when(z + o <= levels - 1)
            def _():
                row_finish(z + o)
                absorb(z + o)

        @pl.when(below)
        def _():
            settle(z - 1 - o)

        @pl.when(above)
        def _():
            settle(z + 1 + o)

    far_below = z - (levels - 1) >= 0
    far_above = z + levels - 1 <= levels - 1

    @pl.when(far_below)
    def _():
        absorb(z - (levels - 1))

    @pl.when(far_above)
    def _():
        absorb(z + levels - 1)

    start = jnp.zeros((LEAD, half + tile), F32)
    for level in range(levels):
        for kk in range(2):
            at = (level * 2 + kk) * deep
            for a in range(2):
                start = start + jnp.dot(
                    lead_all[level, kk, a], natural[1 - a, at : at + deep, :],
                    preferred_element_type=F32,
                )
    panel[...] = 0.5 * start
    vw[...] = jnp.zeros_like(vw)
    diagonal[...] = jnp.zeros_like(diagonal)
    offdiag[...] = jnp.zeros_like(offdiag)

    wide = half + tile
    lane = lax.broadcasted_iota(jnp.int32, (1, wide), 1)
    own_tile = lax.div(lane, tile)
    inside = lane - own_tile * tile
    pos = jnp.where(lane < half, (own_tile * row_count + part) * tile + inside, lane - half)
    lane1 = lax.broadcasted_iota(jnp.int32, (1, tile), 1)
    lane2 = lax.broadcasted_iota(jnp.int32, (2 * PB, tile), 1)
    sub2 = lax.broadcasted_iota(jnp.int32, (2 * PB, tile), 0)
    group_row = lax.broadcasted_iota(jnp.int32, (group, 2 * gvecs + tile), 0)
    sub8 = lax.broadcasted_iota(jnp.int32, (8, half), 0)

    def swap(column):
        return jnp.concatenate([column[PB:], column[:PB]], axis=0)

    def send(slot, d):
        return remote(
            outgoing.at[slot, pl.ds(0, 1)], message.at[slot, pl.ds(part, 1)], msg_send.at[slot, d], msg_recv.at[slot, d], peer(d),
        )


    def rows_late():
        @pl.when(far_below)
        def _():
            row_finish(z - (levels - 1))

        @pl.when(far_above)
        def _():
            row_finish(z + levels - 1)

    def rows_wait():
        for level in range(levels):
            for kk in range(2):
                @pl.when(is_source)
                def _():
                    row_own(level, kk).wait()

                @pl.when(jnp.logical_not(jnp.logical_or(is_source, is_relay)))
                def _():
                    row_relay(level, kk).wait_recv()

    chunk_lanes = half

    def block_work(index):
        at = pl.multiple_of(lax.div(index, 2) * tile, tile)
        to = pl.multiple_of(lax.rem(index, 2) * half, half)

        def rows_of(a):
            return row_all[a, :, :, :, :, pl.ds(at, tile)].reshape(gvecs, tile)

        def cols_of(a):
            return col_all[a, :, :, :, :, pl.ds(to, half)].reshape(gvecs, half)

        correlation[pl.ds(at, tile), pl.ds(to, half)] = inner(rows_of(0), cols_of(0)) * (
            1.0 / gvecs
        )
        reduced[pl.ds(at, tile), pl.ds(to, half)] = 0.5 * (
            inner(rows_of(0), cols_of(1)) + inner(rows_of(1), cols_of(0))
        )

    def swap_copy(level):
        return remote(
            give.at[level], take.at[level], swap_send.at[level], swap_recv.at[level], sib
        )

    def sum_copy(d):
        level = lax.rem(z + d, levels)
        return remote(
            keep.at[level], inbox.at[d], sum_send.at[d], sum_recv.at[d], along(d)
        )

    def rotate(index):
        level = lax.rem(z + 1 + index, levels)
        for kk, target in ((k, keep), (1 - k, give)):
            rows = row_all[0, level, kk].reshape(deep, half)
            target[level] = jnp.dot(rows, eig[...], preferred_element_type=F32)
        swap_copy(level).start()

    def combine(d):
        level = lax.rem(z + d, levels)
        swap_copy(level).wait_recv()
        keep[level] = keep[level] + take[level]
        if d < levels:
            sum_copy(d).start()

    def gather_sums():
        result = keep[z]
        for d in range(1, levels):
            sum_copy(d).wait_recv()
            result = result + inbox[d]
        inbox[0] = result
        moves = []
        for g in range(col_tiles):
            moves.append(pltpu.make_async_copy(
                inbox.at[0, :, g * tile : (g + 1) * tile], spun.at[:, g], spin_sem.at[g]
            ))
        for move in moves:
            move.start()
        for move in moves:
            move.wait()
        rotated[...] = spun[...].astype(BF16)

    def background(step):
        @pl.when(step == 0)
        def _():
            rows_late()

        @pl.when(step == 2)
        def _():
            rows_wait()

        @pl.when(jnp.logical_and(step > 2, step < 3 + levels))
        def _():
            rotate(step - 3)

        for d in range(1, levels + 1):
            @pl.when(step == 3 + d)
            def _():
                combine(d)

        @pl.when(jnp.logical_and(step > 4, step < 5 + 2 * row_tiles))
        def _():
            block_work(step - 5)

        @pl.when(step == PB - 2)
        def _():
            gather_sums()

    @pl.loop(0, PB)
    def _(step):
        slot = lax.rem(step, 2)
        both = vw[...]
        lead_vw = both[:, half:]
        head = lanes_sum(jnp.where(lane2 == step, lead_vw, 0.0))
        column = panel[pl.ds(step, 1), :] - rows_sum(both * swap(head))
        below = pos > step + 1
        masked = jnp.where(below, column, 0.0)[:, :half]
        high, middle, low = parts_of(masked)
        stacked = jnp.where(
            sub8 == 0, high, jnp.where(sub8 == 1, middle, jnp.where(sub8 == 2, low, 0.0))
        ).astype(BF16)
        images = []
        for a in range(2):
            image = rows_sum(jnp.dot(stacked, turned[a], preferred_element_type=F32))
            outgoing[slot, 0:1, a * gvecs : (a + 1) * gvecs] = image
            images.append(image)
        onto = lanes_sum(both[:, :half] * masked)
        tail = lanes_sum(masked * masked)
        small = rows_sum(jnp.where(lane2 == sub2, onto, 0.0)) + jnp.where(
            lane1 == 2 * PB, tail, 0.0
        )
        outgoing[slot, 0:1, 2 * gvecs : 2 * gvecs + tile] = small
        mine = jnp.concatenate(images + [small], axis=1)
        sent = [send(slot, d) for d in range(1, group)]
        for copy in sent:
            copy.start()
        background(step)
        lead_column = column[:, half:]
        pivot = lanes_sum(jnp.where(lane1 == step + 1, lead_column, 0.0))
        here = lanes_sum(jnp.where(lane1 == step, lead_column, 0.0))
        next_row = panel[pl.ds(step + 1, 1), :]
        corner = lanes_sum(jnp.where(lane1 == step + 1, next_row[:, half:], 0.0))
        head_next = lanes_sum(jnp.where(lane2 == step + 1, lead_vw, 0.0))
        for copy in sent:
            copy.wait()
        received = message[slot] + jnp.where(group_row == part, mine, 0.0)
        sums = received[:, : 2 * gvecs]
        pieces = jnp.concatenate(parts_of(sums) + (jnp.zeros_like(sums),), axis=0)
        pieces = pieces.astype(BF16)
        product = rows_sum(
            jnp.dot(pieces[:, :gvecs], natural[1], preferred_element_type=F32)
            + jnp.dot(pieces[:, gvecs:], natural[0], preferred_element_type=F32)
        ) * 0.5
        whole_sum = rows_sum(sums)
        square = lanes_sum(whole_sum[:, :gvecs] * whole_sum[:, gvecs:])
        small = rows_sum(received[:, 2 * gvecs :])
        tail = lanes_sum(jnp.where(lane1 == 2 * PB, small, 0.0))
        onto = lanes_sum(jnp.where(lane2 == sub2, small, 0.0))
        length = jnp.sqrt(pivot * pivot + tail)
        beta = jnp.where(pivot >= 0.0, -length, length)
        tau = (beta - pivot) / beta
        inverse = 1.0 / (pivot - beta)
        vector = jnp.where(
            pos == step + 1, 1.0, jnp.where(below, column * inverse, 0.0)
        )
        onto = onto * inverse + head_next
        image = tau * (product * inverse + next_row - rows_sum(both * swap(onto)))
        edge = lanes_sum(jnp.where(lane1 == step + 1, product[:, half:], 0.0))
        energy = square * inverse * inverse + 2.0 * inverse * edge + corner
        overlap = tau * (energy - 2.0 * rows_sum(onto[:PB] * onto[PB:]))
        image = image - 0.5 * tau * overlap * vector
        vw[pl.ds(step, 1), :] = vector
        vw[pl.ds(PB + step, 1), :] = image
        diagonal[...] = jnp.where(lane1 == step, here, diagonal[...])
        offdiag[...] = jnp.where(lane1 == step, beta, offdiag[...])

    final = vw[:, 0:half]
    right[pl.ds(k, 1)] = final[None]
    trade = remote(
        right.at[k], right.at[k], end_send.at[col_count], end_recv.at[1], (r + 1 - 2 * k, c)
    )
    trade.start()

    def to_row(j):
        return remote(
            right.at[k], left, end_send.at[j], end_recv.at[0], (part, j)
        )

    mine = jnp.logical_and(part >= 2 * z, part < 2 * z + 2)
    for j in range(col_count):
        @pl.when(jnp.logical_and(mine, jnp.logical_not(jnp.logical_and(part == r, c == j))))
        def _():
            to_row(j).start()

    @pl.when(part == r)
    def _():
        left[...] = final

    @pl.when(part != r)
    def _():
        to_row(0).wait_recv()

    trade_in = remote(
        right.at[1 - k], right.at[1 - k], end_send.at[col_count], end_recv.at[1], (r, c)
    )
    trade_in.wait_recv()
    trade.wait_send()
    for j in range(col_count):
        @pl.when(jnp.logical_and(mine, jnp.logical_not(jnp.logical_and(part == r, c == j))))
        def _():
            to_row(j).wait_send()

    for level in range(levels):
        swap_copy(level).wait_send()
    for d in range(1, levels):
        sum_copy(d).wait_send()

    for level in range(levels):
        for kk in range(2):
            @pl.when(is_source)
            def _():
                for i in range(fan):
                    row_out(level, kk, i).wait_send()

            @pl.when(is_relay)
            def _():
                row_relay(level, kk).wait_send()

    @pl.when(c == 0)
    def _():
        for d in range(1, levels):
            lead_z(d).wait_send()
        for d in range(levels):
            each_peer(lambda q: lead_plane(d, q).wait_send())

    for d in range(1, col_count):
        first(d).wait_send()
    for o in range(levels):
        for d in range(col_count):
            @pl.when(jnp.logical_and(not_top, z - o >= 0))
            def _():
                up(o, d).wait_send()

            @pl.when(jnp.logical_and(not_bottom, z + o <= levels - 1))
            def _():
                down(o, d).wait_send()

    for level in range(levels):
        for d in range(col_count):
            across(level, d).wait_send()


def step(psi, hpsi, eig, sizes):
    row_count, col_count, row_tiles, col_tiles, tile = sizes
    g_rows = psi.shape[0]
    half = row_tiles * tile
    levels = row_count // 2
    gvecs = row_count * col_count * g_rows
    deep = gvecs // row_count
    group = 2 * col_count
    whole = pl.BlockSpec(memory_space=pltpu.VMEM)
    dma = pltpu.SemaphoreType.DMA
    return pl.pallas_call(
        functools.partial(step_kernel, sizes),
        out_shape=(
            jax.ShapeDtypeStruct((half, col_tiles * tile), F32),
            jax.ShapeDtypeStruct((half, col_tiles * tile), F32),
            jax.ShapeDtypeStruct((2 * PB, half), F32),
            jax.ShapeDtypeStruct((2, 2 * PB, half), F32),
            jax.ShapeDtypeStruct((1, tile), F32),
            jax.ShapeDtypeStruct((1, tile), F32),
            jax.ShapeDtypeStruct((deep, col_tiles, tile), BF16),
        ),
        in_specs=[whole] * 3,
        out_specs=(whole,) * 7,
        scratch_shapes=[
            pltpu.VMEM((2, levels, 2, col_count, g_rows, col_tiles * tile), BF16),
            pltpu.VMEM((2, levels, 2, col_count, g_rows, half), BF16),
            pltpu.VMEM((levels, 2, 2, LEAD, deep), BF16),
            pltpu.VMEM((col_count, 2, g_rows, col_tiles * tile), BF16),
            pltpu.VMEM((2, gvecs, half + tile), BF16),
            pltpu.VMEM((2, half, gvecs), BF16),
            pltpu.VMEM((LEAD, half + tile), F32),
            pltpu.VMEM((2 * PB, half + tile), F32),
            pltpu.VMEM((2, group, 2 * gvecs + tile), F32),
            pltpu.VMEM((2, 8, 2 * gvecs + tile), F32),
            pltpu.VMEM((levels, deep, col_tiles * tile), F32),
            pltpu.VMEM((levels, deep, col_tiles * tile), F32),
            pltpu.VMEM((levels, deep, col_tiles * tile), F32),
            pltpu.VMEM((levels, deep, col_tiles * tile), F32),
            pltpu.VMEM((deep, col_tiles, tile), F32),
            dma((col_count,)), dma((col_count,)),
            dma((levels, col_count)), dma((levels, col_count)),
            dma((levels, col_count)), dma((levels, col_count)),
            dma((levels, col_count)), dma((levels, col_count)),
            dma((levels,)), dma((levels,)),
            dma((levels, group)), dma((levels, 2)),
            dma((levels, 2, col_count // 2)), dma((levels, 2)),
            dma((levels, 2)),
            dma((2, group)), dma((2, group)),
            dma((col_count + 1,)), dma((2,)),
            dma((levels,)), dma((levels,)),
            dma((levels,)), dma((levels,)),
            dma((col_tiles,)),
        ],
        compiler_params=pltpu.CompilerParams(
            collective_id=0, has_side_effects=True, vmem_limit_bytes=56 * 1024 * 1024
        ),
        cost_estimate=pl.CostEstimate(
            flops=400_000_000, bytes_accessed=4_000_000, transcendentals=0
        ),
        name="step",
    )(psi, hpsi, eig)


def finish_kernel(sizes, reduced, correlation, left, right, updated_out, corr_out, updated, sems):
    row_count, col_count, row_tiles, col_tiles, tile = sizes

    def place(position):
        return 2 * (position % row_tiles) + position // row_tiles

    moves = []
    for position in range(col_tiles):
        move = pltpu.make_async_copy(
            correlation.at[:, position * tile : (position + 1) * tile],
            corr_out.at[:, place(position)], sems.at[position],
        )
        move.start()
        moves.append(move)
    high, middle, low = parts_of(left[...])
    lhs = jnp.concatenate([high, high, middle, middle, high, low], axis=0).astype(BF16)
    for parity in range(2):
        other = right[parity]
        other = jnp.concatenate([other[PB:], other[:PB]], axis=0)
        high, middle, low = parts_of(other)
        rhs = jnp.concatenate([high, middle, high, middle, low, high], axis=0).astype(BF16)
        width = row_tiles * tile
        at = parity * width
        updated[:, at : at + width] = reduced[:, at : at + width] - inner(lhs, rhs)
        for t in range(row_tiles):
            position = parity * row_tiles + t
            move = pltpu.make_async_copy(
                updated.at[:, position * tile : (position + 1) * tile],
                updated_out.at[:, place(position)], sems.at[col_tiles + position],
            )
            move.start()
            moves.append(move)
    for move in moves:
        move.wait()


def finish(reduced, correlation, left, right, sizes):
    row_count, col_count, row_tiles, col_tiles, tile = sizes
    whole = pl.BlockSpec(memory_space=pltpu.VMEM)
    shape = (row_tiles * tile, col_tiles, tile)
    return pl.pallas_call(
        functools.partial(finish_kernel, sizes),
        out_shape=(jax.ShapeDtypeStruct(shape, F32), jax.ShapeDtypeStruct(shape, F32)),
        in_specs=[whole] * 4,
        out_specs=(pl.BlockSpec(memory_space=pl.ANY),) * 2,
        scratch_shapes=[
            pltpu.VMEM((row_tiles * tile, col_tiles * tile), F32),
            pltpu.SemaphoreType.DMA((2 * col_tiles,)),
        ],
        cost_estimate=pl.CostEstimate(
            flops=200_000_000, bytes_accessed=8_000_000, transcendentals=0
        ),
        name="finish",
    )(reduced, correlation, left, right)


def on_device(psi, hpsi, eigvec):
    row_tiles = eigvec.shape[0]
    tile = eigvec.shape[2]
    col_tiles = eigvec.shape[3]
    row_count = lax.axis_size("row")
    col_count = lax.axis_size("col")
    sizes = (row_count, col_count, row_tiles, col_tiles, tile)
    flat = eigvec.reshape(row_tiles * tile, col_tiles * tile)
    reduced, correlation, left, right, diagonal, offdiag, rotated = step(psi, hpsi, flat, sizes)
    updated, correlation = finish(reduced, correlation, left, right, sizes)
    tile_shape = (row_tiles, 1, tile, col_tiles, 1, tile)
    return (
        correlation.reshape(tile_shape),
        updated.reshape(tile_shape),
        diagonal[0, :PB],
        offdiag[0, :PB],
        rotated.reshape(rotated.shape[0], col_tiles, 1, tile),
    )


def solution(mesh):
    return jax.shard_map(
        on_device,
        mesh=mesh,
        in_specs=(
            P(("row", "col"), None),
            P(("row", "col"), None),
            P(None, "row", None, None, "col", None),
        ),
        out_specs=(
            P(None, "row", None, None, "col", None),
            P(None, "row", None, None, "col", None),
            P(),
            P(),
            P("row", None, "col", None),
        ),
        check_vma=False,
    )
```

```python
import functools

import jax
import jax.numpy as jnp
from jax import lax
from jax.experimental import pallas as pl
from jax.experimental.pallas import tpu as pltpu
from jax.sharding import PartitionSpec as P

PB = 16
LEAD = 32
F32 = jnp.float32
BF16 = jnp.bfloat16
MESH = pl.DeviceIdType.MESH


def inner(left, right):
    return lax.dot_general(
        left, right, (((0,), (0,)), ((), ())), preferred_element_type=F32
    )


def remote(source, target, send, recv, device):
    return pltpu.make_async_remote_copy(
        src_ref=source, dst_ref=target, send_sem=send, recv_sem=recv,
        device_id=device, device_id_type=MESH,
    )


def enter(devices):
    barrier = pltpu.get_barrier_semaphore()
    for device in devices:
        pl.semaphore_signal(barrier, inc=1, device_id=device, device_id_type=MESH)
    pl.semaphore_wait(barrier, len(devices))


def lanes_sum(array):
    return jnp.sum(array, axis=1, keepdims=True)


def rows_sum(array):
    return jnp.sum(array, axis=0, keepdims=True)


def parts_of(array):
    high = array.astype(BF16).astype(F32)
    rest = array - high
    middle = rest.astype(BF16).astype(F32)
    return high, middle, rest - middle


EARLY = 5


def step_kernel(
    sizes, psi, hpsi, eig,
    reduced, ordered, left, right, ends, rotated,
    correlation, col_all, row_all, lead_all, stage, natural, turned, panel, partial, vw,
    message, outgoing, zmessage, zoutgoing, eig_other, keep, inbox, spun, spun_other,
    s1_send, s1_recv, up_send, up_recv, down_send, down_recv, sib_send, sib_recv,
    leadz_send, leadz_recv, leadp_send, leadp_recv, row_send, row_recv, own_sem,
    give_send, give_recv, msg_send, msg_recv, zmsg_send, zmsg_recv,
    end_send, end_recv, eig_send, eig_recv, sum_send, sum_recv, spin_sem, order_sem,
    spin_send, spin_recv,
):
    row_count, col_count, row_tiles, col_tiles, tile = sizes
    levels = row_count // 2
    half = row_tiles * tile
    full = 2 * half
    wide = full + tile
    gvecs = natural.shape[1]
    deep = gvecs // row_count
    pair = 2 * deep
    r = lax.axis_index("row")
    c = lax.axis_index("col")
    z = lax.div(r, 2)
    k = lax.rem(r, 2)
    is_main = k == 1
    sib = (r + 1 - 2 * k, c)
    partner = c + 1 - 2 * lax.rem(c, 2)
    group = 2 * col_count
    flat_id = k * col_count + c

    def peer(d):
        q = lax.rem(flat_id + d, group)
        return (2 * z + lax.div(q, col_count), lax.rem(q, col_count))

    def along(d):
        return (lax.rem(r + 2 * d, row_count), c)

    def turn(d):
        return lax.rem((partner if d % 2 else c) + 2 * (d // 2), col_count)

    def back(d):
        return d if d < 2 else col_count - d + 2 * (d % 2)

    order = [0] + [back(d) for d in range(1, col_count)]

    for target in range(col_count):
        for a, source in enumerate((psi, hpsi)):
            for parity in range(2):
                for t in range(row_tiles):
                    j = target + col_count * parity + row_count * t
                    at = (parity * row_tiles + t) * tile
                    stage[target, a, :, at : at + tile] = source[:, j * tile : (j + 1) * tile]
    col_all[:, z, k, c] = stage[c]
    message[...] = jnp.zeros_like(message)
    zmessage[...] = jnp.zeros_like(zmessage)
    enter([peer(d) for d in range(1, group)] + [along(d) for d in range(1, levels)])

    def first(d):
        return remote(
            stage.at[turn(d)], col_all.at[:, z, k, c], s1_send.at[d], s1_recv.at[d], (r, turn(d))
        )

    def first_in(d):
        place = col_all.at[:, z, k, turn(back(d))]
        return remote(place, place, s1_send.at[d], s1_recv.at[d], (r, turn(d)))

    def across(level, kk, d):
        place = col_all.at[:, level, kk, turn(d)]
        return remote(
            place, place, sib_send.at[level, kk, d], sib_recv.at[level, kk, d], sib
        )

    def eig_copy():
        return remote(eig, eig_other, eig_send.at[0], eig_recv.at[0], sib)

    def row_give(level, kk):
        place = row_all.at[1, :, level, kk]
        return remote(place, place, give_send.at[level, kk], give_recv.at[level, kk], sib)

    def spin_give():
        return remote(spun_other, rotated, spin_send.at[0], spin_recv.at[0], sib)

    def source_c(kc):
        return lax.rem(2 * z + kc, col_count)

    def source_half(kc):
        return lax.div(2 * z + kc, col_count)

    def block_work(index, kc):
        at = pl.multiple_of(lax.div(index, 2) * tile, tile)
        to = pl.multiple_of(lax.rem(index, 2) * half, half)

        def rows_of(a):
            return row_all[kc, a, :, :, :, :, pl.ds(at, tile)].reshape(gvecs, tile)

        def cols_of(a):
            return col_all[a, :, :, :, :, pl.ds(to, half)].reshape(gvecs, half)

        correlation[pl.ds(at, tile), pl.ds(to, half)] = inner(rows_of(0), cols_of(0)) * (
            1.0 / gvecs
        )
        reduced[pl.ds(at, tile), pl.ds(to, half)] = 0.5 * (
            inner(rows_of(0), cols_of(1)) + inner(rows_of(1), cols_of(0))
        )

    def order_copy(position):
        return pltpu.make_async_copy(
            correlation.at[:, position * tile : (position + 1) * tile],
            ordered.at[:, 2 * (position % row_tiles) + position // row_tiles],
            order_sem.at[position],
        )

    def order_start():
        for position in range(col_tiles):
            order_copy(position).start()

    def order_wait():
        for position in range(col_tiles):
            order_copy(position).wait()

    def helper_core():
        not_top = z < levels - 1
        not_bottom = z > 0

        def up(o, kk, d):
            place = col_all.at[:, z - o, kk, turn(d)]
            return remote(place, place, up_send.at[o, kk, d], up_recv.at[o, kk, d], (r + 2, c))

        def up_in(o, kk, d):
            place = col_all.at[:, z - 1 - o, kk, turn(d)]
            return remote(place, place, up_send.at[o, kk, d], up_recv.at[o, kk, d], (r + 2, c))

        def down(o, kk, d):
            place = col_all.at[:, z + o, kk, turn(d)]
            return remote(
                place, place, down_send.at[o, kk, d], down_recv.at[o, kk, d], (r - 2, c)
            )

        def down_in(o, kk, d):
            place = col_all.at[:, z + 1 + o, kk, turn(d)]
            return remote(
                place, place, down_send.at[o, kk, d], down_recv.at[o, kk, d], (r - 2, c)
            )

        def launch(kk, d):
            @pl.when(not_top)
            def _():
                up(0, kk, d).start()

            @pl.when(not_bottom)
            def _():
                down(0, kk, d).start()

        fan = col_count // 2

        def is_source(kc):
            return c == source_c(kc)

        def is_relay(kc):
            return jnp.logical_and(
                c != source_c(kc), lax.rem(c, 2) == lax.rem(source_c(kc), 2)
            )

        def row_from(kc, level, kk):
            lane0 = pl.multiple_of(source_half(kc) * half, half)
            return col_all.at[:, level, kk, :, :, pl.ds(lane0, half)]

        def row_own(kc, level, kk):
            return pltpu.make_async_copy(
                row_from(kc, level, kk), row_all.at[kc, :, level, kk], own_sem.at[kc, level, kk]
            )

        def row_out(kc, level, kk, i):
            device = (r, partner) if i == 0 else (r, lax.rem(c + 2 * i, col_count))
            return remote(
                row_from(kc, level, kk), row_all.at[kc, :, level, kk],
                row_send.at[kc, level, kk, i], row_recv.at[kc, level, kk], device,
            )

        def row_relay(kc, level, kk):
            place = row_all.at[kc, :, level, kk]
            return remote(
                place, place, row_send.at[kc, level, kk, 0], row_recv.at[kc, level, kk],
                (r, partner),
            )

        def row_launch(level):
            for kc in range(2):
                @pl.when(is_source(kc))
                def _():
                    for kk in range(2):
                        for i in range(fan):
                            row_out(kc, level, kk, i).start()
                        row_own(kc, level, kk).start()

        def row_finish(level):
            for kc in range(2):
                @pl.when(is_relay(kc))
                def _():
                    for kk in range(2):
                        row_relay(kc, level, kk).wait_recv()
                        row_relay(kc, level, kk).start()

        for d in order:
            if d != 0:
                first_in(back(d)).wait_recv()
            launch(0, d)
            across(z, 0, d).start()
            across(z, 1, d).wait_recv()
            launch(1, d)
        row_launch(z)
        for o in range(levels - 1):
            below = z - 1 - o >= 0
            above = z + 1 + o <= levels - 1
            for d in order:
                for kk in range(2):
                    @pl.when(below)
                    def _():
                        up_in(o, kk, d).wait_recv()

                        @pl.when(not_top)
                        def _():
                            up(o + 1, kk, d).start()

                        across(z - 1 - o, kk, d).start()

                    @pl.when(above)
                    def _():
                        down_in(o, kk, d).wait_recv()

                        @pl.when(not_bottom)
                        def _():
                            down(o + 1, kk, d).start()

                        across(z + 1 + o, kk, d).start()

            @pl.when(below)
            def _():
                row_launch(z - 1 - o)

            @pl.when(above)
            def _():
                row_launch(z + 1 + o)

            if o == 0:
                row_finish(z)
            else:
                @pl.when(z - o >= 0)
                def _():
                    row_finish(z - o)

                @pl.when(z + o <= levels - 1)
                def _():
                    row_finish(z + o)

        @pl.when(z - (levels - 1) >= 0)
        def _():
            row_finish(z - (levels - 1))

        @pl.when(z + levels - 1 <= levels - 1)
        def _():
            row_finish(z + levels - 1)

        for level in range(levels):
            for kk in range(2):
                for kc in range(2):
                    @pl.when(is_source(kc))
                    def _():
                        row_own(kc, level, kk).wait()

                    @pl.when(jnp.logical_not(jnp.logical_or(is_source(kc), is_relay(kc))))
                    def _():
                        row_relay(kc, level, kk).wait_recv()

                row_give(level, kk).start()
        eig_copy().wait_recv()

        def sum_copy(d):
            return remote(
                keep.at[lax.rem(z + d, levels)], inbox.at[d], sum_send.at[d], sum_recv.at[d],
                along(d),
            )

        for i in range(levels):
            level = lax.rem(z + 1 + i, levels)
            keep[level] = jnp.dot(
                row_all[0, 0, level].reshape(pair, half), eig[...], preferred_element_type=F32
            ) + jnp.dot(
                row_all[1, 0, level].reshape(pair, half), eig_other[...],
                preferred_element_type=F32,
            )
            if i < levels - 1:
                sum_copy(i + 1).start()

        @pl.loop(0, 2 * row_tiles)
        def _(index):
            block_work(index, 0)

        order_start()
        result = keep[z]
        for d in range(1, levels):
            sum_copy(d).wait_recv()
            result = result + inbox[d]
        inbox[0] = result
        moves = []
        for kk in range(2):
            for g in range(col_tiles):
                moves.append(pltpu.make_async_copy(
                    inbox.at[0, kk * deep : (kk + 1) * deep, g * tile : (g + 1) * tile],
                    spun.at[kk, :, g], spin_sem.at[kk, g],
                ))
        for move in moves:
            move.start()
        for move in moves:
            move.wait()
        spun_other[...] = spun[1].astype(BF16)
        spin_give().start()
        rotated[...] = spun[0].astype(BF16)
        order_wait()

        for level in range(levels):
            for kk in range(2):
                for kc in range(2):
                    @pl.when(is_source(kc))
                    def _():
                        for i in range(fan):
                            row_out(kc, level, kk, i).wait_send()

                    @pl.when(is_relay(kc))
                    def _():
                        row_relay(kc, level, kk).wait_send()

                row_give(level, kk).wait_send()
                for d in range(col_count):
                    @pl.when(jnp.logical_or(level != z, kk == 0))
                    def _():
                        across(level, kk, d).wait_send()

        for o in range(levels):
            for kk in range(2):
                for d in range(col_count):
                    @pl.when(jnp.logical_and(not_top, z - o >= 0))
                    def _():
                        up(o, kk, d).wait_send()

                    @pl.when(jnp.logical_and(not_bottom, z + o <= levels - 1))
                    def _():
                        down(o, kk, d).wait_send()

        for d in range(1, levels):
            sum_copy(d).wait_send()
        spin_give().wait_send()
        left_in().wait_recv()
        right_copy().wait_recv()
        ends_copy().wait_recv()

    def left_in():
        return remote(right.at[0], left, end_send.at[0, 0], end_recv.at[0], (r, c))

    def right_copy():
        return remote(right, right, end_send.at[2, 0], end_recv.at[1], sib)

    def ends_copy():
        return remote(ends, ends, end_send.at[2, 1], end_recv.at[2], sib)

    def main_core():
        for d in order:
            if d != 0:
                first_in(back(d)).wait_recv()
            across(z, 1, d).start()
        eig_copy().start()
        for d in order:
            across(z, 0, d).wait_recv()

        def lead_z(d):
            place = lead_all.at[z]
            return remote(place, place, leadz_send.at[d], leadz_recv.at[d], along(d))

        def lead_z_in(d):
            place = lead_all.at[lax.rem(z + levels - d, levels)]
            return remote(place, place, leadz_send.at[d], leadz_recv.at[d], along(d))

        def lead_plane(d, q):
            level = lax.rem(z + levels - d, levels)
            place = lead_all.at[level]
            return remote(place, place, leadp_send.at[d, q], leadp_recv.at[level], (r, q))

        def lead_in(level):
            place = lead_all.at[level]
            return remote(place, place, leadp_send.at[0, 0], leadp_recv.at[level], (r, c))

        @pl.when(c == 0)
        def _():
            for kk in range(2):
                for a in range(2):
                    block = col_all[a, z, kk, :, :, 0:tile].astype(F32).reshape(deep, tile)
                    lead_all[z, kk, a] = jnp.transpose(block)[0:LEAD].astype(BF16)
            for q in range(1, col_count):
                lead_plane(0, q).start()
            for d in range(1, levels):
                lead_z(d).start()

        def absorb_own(level):
            for kk in range(2):
                at = pl.multiple_of((level * 2 + kk) * deep, deep)
                for a in range(2):
                    own = col_all[a, level, kk].reshape(deep, full)
                    natural[a, pl.ds(at, deep), 0:full] = own
                    turned[a, :, pl.ds(at, deep)] = jnp.transpose(own.astype(F32)).astype(BF16)

        def absorb_lead(level):
            for kk in range(2):
                at = pl.multiple_of((level * 2 + kk) * deep, deep)
                for a in range(2):
                    lead = lead_all[level, kk, a].astype(F32)
                    lead = jnp.concatenate(
                        [lead, jnp.zeros((tile - LEAD, deep), F32)], axis=0
                    )
                    natural[a, pl.ds(at, deep), full:wide] = jnp.transpose(lead).astype(BF16)

        def absorb(level):
            for kk in range(2):
                for d in range(col_count):
                    across(level, kk, d).wait_recv()
            absorb_own(level)
            absorb_lead(level)

        def lead_product(level):
            total = jnp.zeros((LEAD, wide), F32)
            for kk in range(2):
                at = pl.multiple_of((level * 2 + kk) * deep, deep)
                for a in range(2):
                    total = total + jnp.dot(
                        lead_all[level, kk, a], natural[1 - a, pl.ds(at, deep), :],
                        preferred_element_type=F32,
                    )
            return 0.5 * total

        absorb_own(z)

        @pl.when(c != 0)
        def _():
            lead_in(z).wait_recv()

        absorb_lead(z)
        partial[...] = lead_product(z)
        vw[...] = jnp.zeros_like(vw)
        ends[...] = jnp.zeros_like(ends)

        lane = lax.broadcasted_iota(jnp.int32, (1, wide), 1)
        own_tile = lax.div(lane, tile)
        inside = lane - own_tile * tile
        parity = lax.div(own_tile, row_tiles)
        band = c + col_count * parity + row_count * (own_tile - row_tiles * parity)
        pos = jnp.where(lane < full, band * tile + inside, lane - full)
        lane1 = lax.broadcasted_iota(jnp.int32, (1, tile), 1)
        lane2 = lax.broadcasted_iota(jnp.int32, (2 * PB, tile), 1)
        sub2 = lax.broadcasted_iota(jnp.int32, (2 * PB, tile), 0)
        sub8 = lax.broadcasted_iota(jnp.int32, (8, full), 0)
        sub1 = lax.broadcasted_iota(jnp.int32, (8, 1), 0)
        zwidth = 2 * wide + tile

        def swap(column):
            return jnp.concatenate([column[PB:], column[:PB]], axis=0)

        def zcopies(slot):
            return [
                remote(
                    zoutgoing.at[slot, pl.ds(0, 1)], zmessage.at[slot, pl.ds(z, 1)],
                    zmsg_send.at[slot, d], zmsg_recv.at[slot, d], along(d),
                )
                for d in range(1, levels)
            ]

        def zsum(slot, pieces):
            mine = jnp.concatenate(pieces, axis=1)
            zoutgoing[slot, 0:1, :] = mine
            copies = zcopies(slot)
            for copy in copies:
                copy.start()
            for copy in copies:
                copy.wait()
            return rows_sum(zmessage[slot] + jnp.where(sub1 == z, mine, 0.0))

        opening = zsum(2, [partial[0:1, :], partial[1:2, :], jnp.zeros((1, tile), F32)])
        panel[0:1, :] = opening[:, :wide]
        panel[1:2, :] = opening[:, wide : 2 * wide]

        def front(step):
            both = vw[...]
            lead_vw = both[:, full:]
            head = lanes_sum(jnp.where(lane2 == step, lead_vw, 0.0))
            column = panel[pl.ds(step, 1), :] - rows_sum(both * swap(head))
            masked = jnp.where(pos > step + 1, column, 0.0)[:, :full]
            high, middle, low = parts_of(masked)
            stacked = jnp.where(
                sub8 == 0, high, jnp.where(sub8 == 1, middle, jnp.where(sub8 == 2, low, 0.0))
            ).astype(BF16)
            return both, column, masked, stacked

        def smalls(both, masked):
            onto = lanes_sum(both[:, :full] * masked)
            tail = lanes_sum(masked * masked)
            return rows_sum(jnp.where(lane2 == sub2, onto, 0.0)) + jnp.where(
                lane1 == 2 * PB, tail, 0.0
            )

        def plane_copies(slot, at):
            return [
                remote(
                    outgoing.at[slot, pl.ds(0, 1), at:], message.at[slot, pl.ds(c, 1), at:],
                    msg_send.at[slot, d], msg_recv.at[slot, d],
                    (r, lax.rem(c + d, col_count)),
                )
                for d in range(1, col_count)
            ]

        def settle(step, both, column, product, square, small):
            lead_column = column[:, full:]
            pivot = lanes_sum(jnp.where(lane1 == step + 1, lead_column, 0.0))
            here = lanes_sum(jnp.where(lane1 == step, lead_column, 0.0))
            next_row = panel[pl.ds(step + 1, 1), :]
            corner = lanes_sum(jnp.where(lane1 == step + 1, next_row[:, full:], 0.0))
            head_next = lanes_sum(jnp.where(lane2 == step + 1, both[:, full:], 0.0))
            tail = lanes_sum(jnp.where(lane1 == 2 * PB, small, 0.0))
            onto = lanes_sum(jnp.where(lane2 == sub2, small, 0.0))
            length = jnp.sqrt(pivot * pivot + tail)
            beta = jnp.where(pivot >= 0.0, -length, length)
            tau = (beta - pivot) / beta
            inverse = 1.0 / (pivot - beta)
            vector = jnp.where(
                pos == step + 1, 1.0, jnp.where(pos > step + 1, column * inverse, 0.0)
            )
            onto = onto * inverse + head_next
            image = tau * (product * inverse + next_row - rows_sum(both * swap(onto)))
            edge = lanes_sum(jnp.where(lane1 == step + 1, product[:, full:], 0.0))
            energy = square * inverse * inverse + 2.0 * inverse * edge + corner
            overlap = tau * (energy - 2.0 * rows_sum(onto[:PB] * onto[PB:]))
            image = image - 0.5 * tau * overlap * vector
            vw[pl.ds(step, 1), :] = vector
            vw[pl.ds(PB + step, 1), :] = image
            ends[0:1, :] = jnp.where(lane1 == step, here, ends[0:1, :])
            ends[1:2, :] = jnp.where(lane1 == step, beta, ends[1:2, :])

        def pieces_of(sums):
            return jnp.concatenate(
                parts_of(sums) + (jnp.zeros_like(sums),), axis=0
            ).astype(BF16)

        near = pl.multiple_of(z * pair, pair)
        early_at = 2 * gvecs - 2 * pair

        def early_background(step):
            @pl.when(step == 0)
            def _():
                @pl.when(c == 0)
                def _():
                    for d in range(1, levels):
                        lead_z_in(d).wait_recv()
                        for q in range(1, col_count):
                            lead_plane(d, q).start()

            @pl.when(step == 2)
            def _():
                @pl.when(c != 0)
                def _():
                    for d in range(1, levels):
                        lead_in(lax.rem(z + d, levels)).wait_recv()

                @pl.when(z >= 1)
                def _():
                    absorb(z - 1)

            @pl.when(step == 3)
            def _():
                @pl.when(z + 1 <= levels - 1)
                def _():
                    absorb(z + 1)

        @pl.loop(0, EARLY)
        def _(step):
            slot = lax.rem(step, 2)
            both, column, masked, stacked = front(step)
            mine = []
            for a in range(2):
                mine.append(rows_sum(jnp.dot(
                    stacked, turned[a, :, pl.ds(near, pair)], preferred_element_type=F32
                )))
            mine.append(smalls(both, masked))
            mine = jnp.concatenate(mine, axis=1)
            outgoing[slot, 0:1, early_at:] = mine
            copies = plane_copies(slot, early_at)
            for copy in copies:
                copy.start()
            early_background(step)
            for copy in copies:
                copy.wait()
            received = message[slot, :, early_at:] + jnp.where(sub1 == c, mine, 0.0)
            sums = received[:, : 2 * pair]
            pieces = pieces_of(sums)
            product = 0.5 * rows_sum(
                jnp.dot(
                    pieces[:, :pair], natural[1, pl.ds(near, pair), :],
                    preferred_element_type=F32,
                )
                + jnp.dot(
                    pieces[:, pair:], natural[0, pl.ds(near, pair), :],
                    preferred_element_type=F32,
                )
            )
            whole_sum = rows_sum(sums)
            square = lanes_sum(whole_sum[:, :pair] * whole_sum[:, pair:])
            small = rows_sum(received[:, 2 * pair :])
            total = zsum(slot, [
                product, partial[pl.ds(step + 2, 1), :], jnp.where(lane1 == 0, square, 0.0),
            ])
            panel[pl.ds(step + 2, 1), :] = total[:, wide : 2 * wide]
            square = lanes_sum(total[:, 2 * wide :])
            settle(step, both, column, total[:, :wide], square, small)

        for o in range(1, levels - 1):
            @pl.when(z - 1 - o >= 0)
            def _():
                absorb(z - 1 - o)

            @pl.when(z + 1 + o <= levels - 1)
            def _():
                absorb(z + 1 + o)

        start = lead_product(0)
        for level in range(1, levels):
            start = start + lead_product(level)
        panel[...] = start

        rows_at = EARLY + 3
        work_at = rows_at + 1

        def background(step):
            @pl.when(step == rows_at)
            def _():
                for level in range(levels):
                    for kk in range(2):
                        row_give(level, kk).wait_recv()

            @pl.when(jnp.logical_and(step >= work_at, step < work_at + row_tiles))
            def _():
                block_work(2 * (step - work_at), 1)
                block_work(2 * (step - work_at) + 1, 1)

            @pl.when(step == work_at + row_tiles)
            def _():
                order_start()

            @pl.when(step == PB - 1)
            def _():
                order_wait()

        @pl.loop(EARLY, PB)
        def _(step):
            slot = lax.rem(step, 2)
            both, column, masked, stacked = front(step)
            mine = []
            for a in range(2):
                mine.append(
                    rows_sum(jnp.dot(stacked, turned[a], preferred_element_type=F32))
                )
            mine.append(smalls(both, masked))
            mine = jnp.concatenate(mine, axis=1)
            outgoing[slot, 0:1, :] = mine
            copies = plane_copies(slot, 0)
            for copy in copies:
                copy.start()
            background(step)
            for copy in copies:
                copy.wait()
            received = message[slot] + jnp.where(sub1 == c, mine, 0.0)
            sums = received[:, : 2 * gvecs]
            pieces = pieces_of(sums)
            product = 0.5 * rows_sum(
                jnp.dot(pieces[:, :gvecs], natural[1], preferred_element_type=F32)
                + jnp.dot(pieces[:, gvecs:], natural[0], preferred_element_type=F32)
            )
            whole_sum = rows_sum(sums)
            square = lanes_sum(whole_sum[:, :gvecs] * whole_sum[:, gvecs:])
            settle(step, both, column, product, square, rows_sum(received[:, 2 * gvecs :]))

        for side in range(2):
            right[side] = vw[:, side * half : (side + 1) * half]

        def left_out(kc, q):
            return remote(
                right.at[source_half(kc)], left, end_send.at[kc, q], end_recv.at[0],
                (2 * z + kc, q),
            )

        def each_left(action):
            for kc in range(2):
                for q in range(col_count):
                    away = c == source_c(kc)
                    if kc == 1:
                        away = jnp.logical_and(away, c != q)

                    @pl.when(away)
                    def _():
                        action(left_out(kc, q))

        each_left(lambda copy: copy.start())
        right_copy().start()
        ends_copy().start()

        @pl.when(c == source_c(1))
        def _():
            left[...] = right[source_half(1)]

        @pl.when(c != source_c(1))
        def _():
            left_in().wait_recv()

        each_left(lambda copy: copy.wait_send())
        right_copy().wait_send()
        ends_copy().wait_send()
        spin_give().wait_recv()
        eig_copy().wait_send()
        for d in range(col_count):
            across(z, 1, d).wait_send()

        @pl.when(c == 0)
        def _():
            for d in range(levels):
                for q in range(1, col_count):
                    lead_plane(d, q).wait_send()
            for d in range(1, levels):
                lead_z(d).wait_send()

    for d in range(1, col_count):
        first(d).start()

    @pl.when(k == 0)
    def _():
        helper_core()

    @pl.when(is_main)
    def _():
        main_core()

    for d in range(1, col_count):
        first(d).wait_send()


def step(psi, hpsi, eig, sizes):
    row_count, col_count, row_tiles, col_tiles, tile = sizes
    g_rows = psi.shape[0]
    half = row_tiles * tile
    full = col_tiles * tile
    wide = full + tile
    levels = row_count // 2
    gvecs = row_count * col_count * g_rows
    deep = gvecs // row_count
    whole = pl.BlockSpec(memory_space=pltpu.VMEM)
    dma = pltpu.SemaphoreType.DMA

    def both(*shape):
        return [dma(shape), dma(shape)]

    return pl.pallas_call(
        functools.partial(step_kernel, sizes),
        out_shape=(
            jax.ShapeDtypeStruct((half, full), F32),
            jax.ShapeDtypeStruct((half, col_tiles, tile), F32),
            jax.ShapeDtypeStruct((2 * PB, half), F32),
            jax.ShapeDtypeStruct((2, 2 * PB, half), F32),
            jax.ShapeDtypeStruct((8, tile), F32),
            jax.ShapeDtypeStruct((deep, col_tiles, tile), BF16),
        ),
        in_specs=[whole] * 3,
        out_specs=(whole,) * 6,
        scratch_shapes=[
            pltpu.VMEM((half, full), F32),
            pltpu.VMEM((2, levels, 2, col_count, g_rows, full), BF16),
            pltpu.VMEM((2, 2, levels, 2, col_count, g_rows, half), BF16),
            pltpu.VMEM((levels, 2, 2, LEAD, deep), BF16),
            pltpu.VMEM((col_count, 2, g_rows, full), BF16),
            pltpu.VMEM((2, gvecs, wide), BF16),
            pltpu.VMEM((2, full, gvecs), BF16),
            pltpu.VMEM((LEAD, wide), F32),
            pltpu.VMEM((LEAD, wide), F32),
            pltpu.VMEM((2 * PB, wide), F32),
            pltpu.VMEM((2, 8, 2 * gvecs + tile), F32),
            pltpu.VMEM((2, 8, 2 * gvecs + tile), F32),
            pltpu.VMEM((3, 8, 2 * wide + tile), F32),
            pltpu.VMEM((3, 8, 2 * wide + tile), F32),
            pltpu.VMEM((half, full), BF16),
            pltpu.VMEM((levels, 2 * deep, full), F32),
            pltpu.VMEM((levels, 2 * deep, full), F32),
            pltpu.VMEM((2, deep, col_tiles, tile), F32),
            pltpu.VMEM((deep, col_tiles, tile), BF16),
            *both(col_count),
            *both(levels, 2, col_count), *both(levels, 2, col_count),
            *both(levels, 2, col_count),
            *both(levels),
            dma((levels, col_count)), dma((levels,)),
            dma((2, levels, 2, col_count // 2)), dma((2, levels, 2)), dma((2, levels, 2)),
            *both(levels, 2),
            *both(2, col_count), *both(3, levels),
            dma((3, col_count)), dma((3,)),
            *both(1), *both(levels),
            dma((2, col_tiles)), dma((col_tiles,)),
            *both(1),
        ],
        compiler_params=pltpu.CompilerParams(
            collective_id=0, has_side_effects=True, vmem_limit_bytes=60 * 1024 * 1024
        ),
        cost_estimate=pl.CostEstimate(
            flops=400_000_000, bytes_accessed=4_000_000, transcendentals=0
        ),
        name="step",
    )(psi, hpsi, eig)


def finish_kernel(
    sizes, reduced, correlation, left, right, ends, rotated,
    updated_out, corr_out, diag_out, off_out, rotated_out, updated, sems,
):
    row_count, col_count, row_tiles, col_tiles, tile = sizes

    def place(position):
        return 2 * (position % row_tiles) + position // row_tiles

    spin = pltpu.make_async_copy(rotated, rotated_out, sems.at[0])
    spin.start()
    diag_out[...] = ends[0:1, :PB]
    off_out[...] = ends[1:2, :PB]
    first = pltpu.make_async_copy(correlation, corr_out, sems.at[1])
    first.start()
    moves = [spin, first]
    high, middle, low = parts_of(left[...])
    lhs = jnp.concatenate([high, high, middle, middle, high, low], axis=0).astype(BF16)
    for parity in range(2):
        other = right[parity]
        other = jnp.concatenate([other[PB:], other[:PB]], axis=0)
        high, middle, low = parts_of(other)
        rhs = jnp.concatenate([high, middle, high, middle, low, high], axis=0).astype(BF16)
        width = row_tiles * tile
        at = parity * width
        updated[:, at : at + width] = reduced[:, at : at + width] - inner(lhs, rhs)
        for t in range(row_tiles):
            position = parity * row_tiles + t
            move = pltpu.make_async_copy(
                updated.at[:, position * tile : (position + 1) * tile],
                updated_out.at[:, place(position)], sems.at[2 + position],
            )
            move.start()
            moves.append(move)
    for move in moves:
        move.wait()


def finish(parts, sizes):
    row_count, col_count, row_tiles, col_tiles, tile = sizes
    whole = pl.BlockSpec(memory_space=pltpu.VMEM)
    hbm = pl.BlockSpec(memory_space=pl.ANY)
    shape = (row_tiles * tile, col_tiles, tile)
    return pl.pallas_call(
        functools.partial(finish_kernel, sizes),
        out_shape=(
            jax.ShapeDtypeStruct(shape, F32), jax.ShapeDtypeStruct(shape, F32),
            jax.ShapeDtypeStruct((1, PB), F32), jax.ShapeDtypeStruct((1, PB), F32),
            jax.ShapeDtypeStruct(parts[-1].shape, BF16),
        ),
        in_specs=[whole] * 6,
        out_specs=(hbm, hbm, whole, whole, hbm),
        scratch_shapes=[
            pltpu.VMEM((row_tiles * tile, col_tiles * tile), F32),
            pltpu.SemaphoreType.DMA((2 + col_tiles,)),
        ],
        cost_estimate=pl.CostEstimate(
            flops=200_000_000, bytes_accessed=8_000_000, transcendentals=0
        ),
        name="finish",
    )(*parts)


def on_device(psi, hpsi, eigvec):
    row_tiles = eigvec.shape[0]
    tile = eigvec.shape[2]
    col_tiles = eigvec.shape[3]
    row_count = lax.axis_size("row")
    col_count = lax.axis_size("col")
    sizes = (row_count, col_count, row_tiles, col_tiles, tile)
    flat = eigvec.reshape(row_tiles * tile, col_tiles * tile)
    parts = step(psi, hpsi, flat, sizes)
    updated, correlation, diagonal, offdiag, rotated = finish(parts, sizes)
    tile_shape = (row_tiles, 1, tile, col_tiles, 1, tile)
    return (
        correlation.reshape(tile_shape),
        updated.reshape(tile_shape),
        diagonal.reshape(PB),
        offdiag.reshape(PB),
        rotated.reshape(rotated.shape[0], col_tiles, 1, tile),
    )


def solution(mesh):
    return jax.shard_map(
        on_device,
        mesh=mesh,
        in_specs=(
            P(("row", "col"), None),
            P(("row", "col"), None),
            P(None, "row", None, None, "col", None),
        ),
        out_specs=(
            P(None, "row", None, None, "col", None),
            P(None, "row", None, None, "col", None),
            P(),
            P(),
            P("row", None, "col", None),
        ),
        check_vma=False,
    )
```

```python
import functools
import math

import jax
import jax.numpy as jnp
from jax import lax
from jax.experimental import pallas as pl
from jax.experimental.pallas import tpu as pltpu
from jax.sharding import PartitionSpec as P

PB = 16
LEAD = 32
F32 = jnp.float32
BF16 = jnp.bfloat16
MESH = pl.DeviceIdType.MESH


def inner(left, right):
    return lax.dot_general(
        left, right, (((0,), (0,)), ((), ())), preferred_element_type=F32
    )


def remote(source, target, send, recv, device):
    return pltpu.make_async_remote_copy(
        src_ref=source, dst_ref=target, send_sem=send, recv_sem=recv,
        device_id=device, device_id_type=MESH,
    )


def lanes_sum(array):
    return jnp.sum(array, axis=1, keepdims=True)


def rows_sum(array):
    return jnp.sum(array, axis=0, keepdims=True)


def parts_of(array):
    high = array.astype(BF16).astype(F32)
    rest = array - high
    middle = rest.astype(BF16).astype(F32)
    return high, middle, rest - middle


EARLY = 4


def step_kernel(
    sizes, psi_in, hpsi_in, eig,
    reduced, ordered, left, right, ends, rotated,
    psi, hpsi, col_all, row_all, lead_all, stage, natural, turned, panel, partial, vw,
    message, outgoing, zmessage, zoutgoing, eig_raw, eig_flat, keep, inbox, spun, spun_other,
    s1_send, s1_recv, up_send, up_recv, down_send, down_recv, sib_send, sib_recv,
    leadz_send, leadz_recv, leadp_send, leadp_recv, row_send, row_recv, own_sem,
    give_send, give_recv, msg_send, msg_recv, zmsg_send, zmsg_recv,
    end_send, end_recv, eig_send, eig_recv, upsum_send, upsum_recv, downsum_send, downsum_recv, load_sem,
    spin_send, spin_recv,
):
    row_count, col_count, row_tiles, col_tiles, tile = sizes
    levels = row_count // 2
    half = row_tiles * tile
    full = 2 * half
    wide = full + tile
    gvecs = natural.shape[1]
    deep = gvecs // row_count
    pair = 2 * deep
    r = lax.axis_index("row")
    c = lax.axis_index("col")
    z = lax.div(r, 2)
    k = lax.rem(r, 2)
    is_main = k == 1
    sib = (r + 1 - 2 * k, c)
    partner = c + 1 - 2 * lax.rem(c, 2)
    group = 2 * col_count
    flat_id = k * col_count + c

    def peer(d):
        q = lax.rem(flat_id + d, group)
        return (2 * z + lax.div(q, col_count), lax.rem(q, col_count))

    def along(d):
        return (lax.rem(r + 2 * d, row_count), c)

    def turn(d):
        return lax.rem((partner if d % 2 else c) + 2 * (d // 2), col_count)

    def back(d):
        return d if d < 2 else col_count - d + 2 * (d % 2)

    order = [0] + [back(d) for d in range(1, col_count)]

    loads = [
        pltpu.make_async_copy(psi_in, psi, load_sem.at[0]),
        pltpu.make_async_copy(hpsi_in, hpsi, load_sem.at[1]),
    ]
    for load in loads:
        load.start()
    message[...] = jnp.zeros_like(message)
    zmessage[...] = jnp.zeros_like(zmessage)
    neighbours = [peer(d) for d in range(1, group)] + [along(d) for d in range(1, levels)]
    barrier = pltpu.get_barrier_semaphore()
    for device in neighbours:
        pl.semaphore_signal(barrier, inc=1, device_id=device, device_id_type=MESH)
    for load in loads:
        load.wait()
    for target in range(col_count):
        for a, source in enumerate((psi, hpsi)):
            for parity in range(2):
                for t in range(row_tiles):
                    j = target + col_count * parity + row_count * t
                    at = (parity * row_tiles + t) * tile
                    stage[target, a, :, at : at + tile] = source[:, j * tile : (j + 1) * tile]
    col_all[:, z, k, c] = stage[c]
    pl.semaphore_wait(barrier, len(neighbours))

    def first(d):
        return remote(
            stage.at[turn(d)], col_all.at[:, z, k, c], s1_send.at[d], s1_recv.at[d], (r, turn(d))
        )

    def first_in(d):
        place = col_all.at[:, z, k, turn(back(d))]
        return remote(place, place, s1_send.at[d], s1_recv.at[d], (r, turn(d)))

    def across(level, kk, d):
        place = col_all.at[:, level, kk, turn(d)]
        return remote(
            place, place, sib_send.at[level, kk, d], sib_recv.at[level, kk, d], sib
        )

    def eig_copy():
        return remote(eig, eig_raw.at[1], eig_send.at[0], eig_recv.at[0], sib)

    def row_give(level, kk):
        place = row_all.at[1, :, level, kk]
        return remote(place, place, give_send.at[level, kk], give_recv.at[level, kk], sib)

    def spin_give():
        return remote(spun_other, rotated, spin_send.at[0], spin_recv.at[0], sib)

    def source_c(kc):
        return lax.rem(2 * z + kc, col_count)

    def source_half(kc):
        return lax.div(2 * z + kc, col_count)

    def block_work(index, kc):
        at = pl.multiple_of(index * tile, tile)

        def rows_of(a):
            return row_all[kc, a, :, :, :, :, pl.ds(at, tile)].reshape(gvecs, tile)

        for side in range(2):
            def cols_of(a):
                return col_all[a, :, :, :, :, side * half : (side + 1) * half].reshape(
                    gvecs, half
                )

            result = inner(rows_of(0), cols_of(0)) * (1.0 / gvecs)
            for t in range(row_tiles):
                ordered[pl.ds(at, tile), 2 * t + side, :] = result[:, t * tile : (t + 1) * tile]
            reduced[pl.ds(at, tile), side * half : (side + 1) * half] = 0.5 * (
                inner(rows_of(0), cols_of(1)) + inner(rows_of(1), cols_of(0))
            )

    def helper_core():
        not_top = z < levels - 1
        not_bottom = z > 0

        def up(o, kk, d):
            place = col_all.at[:, z - o, kk, turn(d)]
            return remote(place, place, up_send.at[o, kk, d], up_recv.at[o, kk, d], (r + 2, c))

        def up_in(o, kk, d):
            place = col_all.at[:, z - 1 - o, kk, turn(d)]
            return remote(place, place, up_send.at[o, kk, d], up_recv.at[o, kk, d], (r + 2, c))

        def down(o, kk, d):
            place = col_all.at[:, z + o, kk, turn(d)]
            return remote(
                place, place, down_send.at[o, kk, d], down_recv.at[o, kk, d], (r - 2, c)
            )

        def down_in(o, kk, d):
            place = col_all.at[:, z + 1 + o, kk, turn(d)]
            return remote(
                place, place, down_send.at[o, kk, d], down_recv.at[o, kk, d], (r - 2, c)
            )

        def launch(kk, d):
            @pl.when(not_top)
            def _():
                up(0, kk, d).start()

            @pl.when(not_bottom)
            def _():
                down(0, kk, d).start()

        fan = col_count // 2

        def is_source(kc):
            return c == source_c(kc)

        def is_relay(kc):
            return jnp.logical_and(
                c != source_c(kc), lax.rem(c, 2) == lax.rem(source_c(kc), 2)
            )

        def row_from(kc, level, kk):
            lane0 = pl.multiple_of(source_half(kc) * half, half)
            return col_all.at[:, level, kk, :, :, pl.ds(lane0, half)]

        def row_own(kc, level, kk):
            return pltpu.make_async_copy(
                row_from(kc, level, kk), row_all.at[kc, :, level, kk], own_sem.at[kc, level, kk]
            )

        def row_part(kc, level, kk, a):
            lane0 = pl.multiple_of(source_half(kc) * half, half)
            return col_all.at[a, level, kk, :, :, pl.ds(lane0, half)]

        def row_out(kc, level, kk, a, i):
            device = (r, partner) if i == 0 else (r, lax.rem(c + 2 * i, col_count))
            return remote(
                row_part(kc, level, kk, a), row_all.at[kc, a, level, kk],
                row_send.at[kc, level, kk, a, i], row_recv.at[kc, level, kk, a], device,
            )

        def row_relay(kc, level, kk, a):
            place = row_all.at[kc, a, level, kk]
            return remote(
                place, place, row_send.at[kc, level, kk, a, 0],
                row_recv.at[kc, level, kk, a], (r, partner),
            )

        def row_launch(level):
            for kc in range(2):
                @pl.when(is_source(kc))
                def _():
                    for a in range(2):
                        for kk in range(2):
                            for i in range(fan):
                                row_out(kc, level, kk, a, i).start()
                    for kk in range(2):
                        row_own(kc, level, kk).start()

        def row_finish(level):
            for a in range(2):
                for kk in range(2):
                    for kc in range(2):
                        @pl.when(is_relay(kc))
                        def _():
                            row_relay(kc, level, kk, a).wait_recv()
                            row_relay(kc, level, kk, a).start()

        for d in order:
            if d != 0:
                first_in(back(d)).wait_recv()
            launch(0, d)
            across(z, 0, d).start()
            across(z, 1, d).wait_recv()
            launch(1, d)
        row_launch(z)
        own_eig = pltpu.make_async_copy(eig, eig_raw.at[0], load_sem.at[0])
        own_eig.start()
        own_eig.wait()
        eig_copy().wait_recv()
        for kc in range(2):
            values = eig_raw[kc].astype(F32)
            for g in range(col_tiles):
                eig_flat[kc, :, g * tile : (g + 1) * tile] = values[:, g, :].astype(BF16)
        for o in range(levels - 1):
            below = z - 1 - o >= 0
            above = z + 1 + o <= levels - 1
            for d in order:
                for kk in range(2):
                    @pl.when(below)
                    def _():
                        up_in(o, kk, d).wait_recv()

                        @pl.when(not_top)
                        def _():
                            up(o + 1, kk, d).start()

                        across(z - 1 - o, kk, d).start()

                    @pl.when(above)
                    def _():
                        down_in(o, kk, d).wait_recv()

                        @pl.when(not_bottom)
                        def _():
                            down(o + 1, kk, d).start()

                        across(z + 1 + o, kk, d).start()

            @pl.when(below)
            def _():
                row_launch(z - 1 - o)

            @pl.when(above)
            def _():
                row_launch(z + 1 + o)

            if o == 0:
                row_finish(z)
            else:
                @pl.when(z - o >= 0)
                def _():
                    row_finish(z - o)

                @pl.when(z + o <= levels - 1)
                def _():
                    row_finish(z + o)

        @pl.when(z - (levels - 1) >= 0)
        def _():
            row_finish(z - (levels - 1))

        @pl.when(z + levels - 1 <= levels - 1)
        def _():
            row_finish(z + levels - 1)

        def row_wait(a):
            for level in range(levels):
                for kk in range(2):
                    for kc in range(2):
                        @pl.when(jnp.logical_not(jnp.logical_or(is_source(kc), is_relay(kc))))
                        def _():
                            row_relay(kc, level, kk, a).wait_recv()

        for level in range(levels):
            for kk in range(2):
                for kc in range(2):
                    @pl.when(is_source(kc))
                    def _():
                        row_own(kc, level, kk).wait()

        row_wait(0)

        def upsum(level):
            return remote(
                keep.at[level], inbox.at[level], upsum_send.at[level], upsum_recv.at[level],
                (r + 2, c),
            )

        def downsum(level, place):
            return remote(
                keep.at[level], inbox.at[place], downsum_send.at[level],
                downsum_recv.at[level], (r - 2, c),
            )

        def partial_sum(level):
            keep[level] = jnp.dot(
                row_all[0, 0, level].reshape(pair, half), eig_flat[0],
                preferred_element_type=F32,
            ) + jnp.dot(
                row_all[1, 0, level].reshape(pair, half), eig_flat[1],
                preferred_element_type=F32,
            )

        def send_down(level):
            @pl.when(z - 1 == level)
            def _():
                downsum(level, levels).start()

            @pl.when(z - 1 != level)
            def _():
                downsum(level, level).start()

        for i in range(levels - 1):
            high, low = levels - 1 - i, i

            @pl.when(z < high)
            def _():
                partial_sum(high)

                @pl.when(z == 0)
                def _():
                    upsum(high).start()

            @pl.when(z > low)
            def _():
                partial_sum(low)

                @pl.when(z == levels - 1)
                def _():
                    send_down(low)

        partial_sum(z)
        row_wait(1)
        for level in range(levels):
            for kk in range(2):
                row_give(level, kk).start()

        @pl.loop(0, row_tiles)
        def _(index):
            block_work(index, 0)

        def pass_up(high):
            @pl.when(jnp.logical_and(z > 0, z < high))
            def _():
                upsum(high).wait_recv()
                keep[high] = keep[high] + inbox[high]
                upsum(high).start()

        def pass_down(low):
            @pl.when(jnp.logical_and(z < levels - 1, z > low))
            def _():
                downsum(low, low).wait_recv()
                keep[low] = keep[low] + inbox[low]
                send_down(low)

        @pl.when(z < levels // 2)
        def _():
            for i in range(levels - 1):
                pass_up(levels - 1 - i)
                pass_down(i)

        @pl.when(z >= levels // 2)
        def _():
            for i in range(levels - 1):
                pass_down(i)
                pass_up(levels - 1 - i)

        @pl.when(z > 0)
        def _():
            upsum(z).wait_recv()
            keep[z] = keep[z] + inbox[z]

        @pl.when(z < levels - 1)
        def _():
            downsum(z, levels).wait_recv()
            keep[z] = keep[z] + inbox[levels]

        for kk in (1, 0):
            for g in range(col_tiles):
                spun[:, g, :] = keep[z, kk * deep : (kk + 1) * deep, g * tile : (g + 1) * tile]
            if kk:
                spun_other[...] = spun[...].astype(BF16)
                spin_give().start()
            else:
                rotated[...] = spun[...].astype(BF16)

        for level in range(levels):
            for kk in range(2):
                for kc in range(2):
                    for a in range(2):
                        @pl.when(is_source(kc))
                        def _():
                            for i in range(fan):
                                row_out(kc, level, kk, a, i).wait_send()

                        @pl.when(is_relay(kc))
                        def _():
                            row_relay(kc, level, kk, a).wait_send()

                row_give(level, kk).wait_send()
                for d in range(col_count):
                    @pl.when(jnp.logical_or(level != z, kk == 0))
                    def _():
                        across(level, kk, d).wait_send()

        for o in range(levels):
            for kk in range(2):
                for d in range(col_count):
                    @pl.when(jnp.logical_and(not_top, z - o >= 0))
                    def _():
                        up(o, kk, d).wait_send()

                    @pl.when(jnp.logical_and(not_bottom, z + o <= levels - 1))
                    def _():
                        down(o, kk, d).wait_send()

        for level in range(levels):
            @pl.when(z < level)
            def _():
                upsum(level).wait_send()

            @pl.when(z > level)
            def _():
                downsum(level, level).wait_send()

        spin_give().wait_send()
        left_in().wait_recv()
        right_copy().wait_recv()
        ends_copy().wait_recv()

    def left_in():
        return remote(right.at[0], left, end_send.at[0, 0], end_recv.at[0], (r, c))

    def right_copy():
        return remote(right, right, end_send.at[2, 0], end_recv.at[1], sib)

    def ends_copy():
        return remote(ends, ends, end_send.at[2, 1], end_recv.at[2], sib)

    def main_core():
        for d in order:
            if d != 0:
                first_in(back(d)).wait_recv()
            across(z, 1, d).start()
        eig_copy().start()
        for d in order:
            across(z, 0, d).wait_recv()

        def lead_z(d):
            place = lead_all.at[z]
            return remote(place, place, leadz_send.at[d], leadz_recv.at[d], along(d))

        def lead_z_in(d):
            place = lead_all.at[lax.rem(z + levels - d, levels)]
            return remote(place, place, leadz_send.at[d], leadz_recv.at[d], along(d))

        def lead_plane(d, q):
            level = lax.rem(z + levels - d, levels)
            place = lead_all.at[level]
            return remote(place, place, leadp_send.at[d, q], leadp_recv.at[level], (r, q))

        def lead_in(level):
            place = lead_all.at[level]
            return remote(place, place, leadp_send.at[0, 0], leadp_recv.at[level], (r, c))

        @pl.when(c == 0)
        def _():
            for kk in range(2):
                for a in range(2):
                    block = col_all[a, z, kk, :, :, 0:tile].astype(F32).reshape(deep, tile)
                    lead_all[z, kk, a] = jnp.transpose(block)[0:LEAD].astype(BF16)
            for q in range(1, col_count):
                lead_plane(0, q).start()
            for d in range(1, levels):
                lead_z(d).start()

        def absorb_own(level):
            for kk in range(2):
                at = pl.multiple_of((level * 2 + kk) * deep, deep)
                for a in range(2):
                    own = col_all[a, level, kk].reshape(deep, full)
                    natural[a, pl.ds(at, deep), 0:full] = own
                    turned[a, :, pl.ds(at, deep)] = jnp.transpose(own.astype(F32)).astype(BF16)

        def absorb_lead(level):
            for kk in range(2):
                at = pl.multiple_of((level * 2 + kk) * deep, deep)
                for a in range(2):
                    lead = lead_all[level, kk, a].astype(F32)
                    lead = jnp.concatenate(
                        [lead, jnp.zeros((tile - LEAD, deep), F32)], axis=0
                    )
                    natural[a, pl.ds(at, deep), full:wide] = jnp.transpose(lead).astype(BF16)

        def absorb(level):
            for kk in range(2):
                for d in range(col_count):
                    across(level, kk, d).wait_recv()
            absorb_own(level)
            absorb_lead(level)

        def lead_product(level):
            total = jnp.zeros((LEAD, wide), F32)
            for kk in range(2):
                at = pl.multiple_of((level * 2 + kk) * deep, deep)
                for a in range(2):
                    total = total + jnp.dot(
                        lead_all[level, kk, a], natural[1 - a, pl.ds(at, deep), :],
                        preferred_element_type=F32,
                    )
            return 0.5 * total

        absorb_own(z)

        @pl.when(c != 0)
        def _():
            lead_in(z).wait_recv()

        absorb_lead(z)
        partial[...] = lead_product(z)
        vw[...] = jnp.zeros_like(vw)
        ends[...] = jnp.zeros_like(ends)

        lane = lax.broadcasted_iota(jnp.int32, (1, wide), 1)
        own_tile = lax.div(lane, tile)
        inside = lane - own_tile * tile
        parity = lax.div(own_tile, row_tiles)
        band = c + col_count * parity + row_count * (own_tile - row_tiles * parity)
        pos = jnp.where(lane < full, band * tile + inside, lane - full)
        lane1 = lax.broadcasted_iota(jnp.int32, (1, tile), 1)
        lane2 = lax.broadcasted_iota(jnp.int32, (2 * PB, tile), 1)
        sub2 = lax.broadcasted_iota(jnp.int32, (2 * PB, tile), 0)
        sub8 = lax.broadcasted_iota(jnp.int32, (8, full), 0)
        sub1 = lax.broadcasted_iota(jnp.int32, (8, 1), 0)
        zwidth = 2 * wide + tile

        def swap(column):
            return jnp.concatenate([column[PB:], column[:PB]], axis=0)

        def zcopies(slot):
            return [
                remote(
                    zoutgoing.at[slot, pl.ds(0, 1)], zmessage.at[slot, pl.ds(z, 1)],
                    zmsg_send.at[slot, d], zmsg_recv.at[slot, d], along(d),
                )
                for d in range(1, levels)
            ]

        def zsum(slot, pieces):
            mine = jnp.concatenate(pieces, axis=1)
            zoutgoing[slot, 0:1, :] = mine
            copies = zcopies(slot)
            for copy in copies:
                copy.start()
            for copy in copies:
                copy.wait()
            return rows_sum(zmessage[slot] + jnp.where(sub1 == z, mine, 0.0))

        opening = zsum(2, [partial[0:1, :], partial[1:2, :], jnp.zeros((1, tile), F32)])
        panel[0:1, :] = opening[:, :wide]
        panel[1:2, :] = opening[:, wide : 2 * wide]

        def front(step):
            both = vw[...]
            lead_vw = both[:, full:]
            head = lanes_sum(jnp.where(lane2 == step, lead_vw, 0.0))
            column = panel[pl.ds(step, 1), :] - rows_sum(both * swap(head))
            masked = jnp.where(pos > step + 1, column, 0.0)[:, :full]
            high, middle, low = parts_of(masked)
            stacked = jnp.where(
                sub8 == 0, high, jnp.where(sub8 == 1, middle, jnp.where(sub8 == 2, low, 0.0))
            ).astype(BF16)
            return both, column, masked, stacked

        def smalls(both, masked):
            onto = lanes_sum(both[:, :full] * masked)
            tail = lanes_sum(masked * masked)
            return rows_sum(jnp.where(lane2 == sub2, onto, 0.0)) + jnp.where(
                lane1 == 2 * PB, tail, 0.0
            )

        def plane_copies(slot, at):
            return [
                remote(
                    outgoing.at[slot, pl.ds(0, 1), at:], message.at[slot, pl.ds(c, 1), at:],
                    msg_send.at[slot, d], msg_recv.at[slot, d],
                    (r, lax.rem(c + d, col_count)),
                )
                for d in range(1, col_count)
            ]

        def settle(step, both, column, product, square, small):
            lead_column = column[:, full:]
            pivot = lanes_sum(jnp.where(lane1 == step + 1, lead_column, 0.0))
            here = lanes_sum(jnp.where(lane1 == step, lead_column, 0.0))
            next_row = panel[pl.ds(step + 1, 1), :]
            corner = lanes_sum(jnp.where(lane1 == step + 1, next_row[:, full:], 0.0))
            head_next = lanes_sum(jnp.where(lane2 == step + 1, both[:, full:], 0.0))
            tail = lanes_sum(jnp.where(lane1 == 2 * PB, small, 0.0))
            onto = lanes_sum(jnp.where(lane2 == sub2, small, 0.0))
            length = jnp.sqrt(pivot * pivot + tail)
            beta = jnp.where(pivot >= 0.0, -length, length)
            tau = (beta - pivot) / beta
            inverse = 1.0 / (pivot - beta)
            vector = jnp.where(
                pos == step + 1, 1.0, jnp.where(pos > step + 1, column * inverse, 0.0)
            )
            onto = onto * inverse + head_next
            image = tau * (product * inverse + next_row - rows_sum(both * swap(onto)))
            edge = lanes_sum(jnp.where(lane1 == step + 1, product[:, full:], 0.0))
            energy = square * inverse * inverse + 2.0 * inverse * edge + corner
            overlap = tau * (energy - 2.0 * rows_sum(onto[:PB] * onto[PB:]))
            image = image - 0.5 * tau * overlap * vector
            vw[pl.ds(step, 1), :] = vector
            vw[pl.ds(PB + step, 1), :] = image
            ends[0:1, :] = jnp.where(lane1 == step, here, ends[0:1, :])
            ends[1:2, :] = jnp.where(lane1 == step, beta, ends[1:2, :])

        def pieces_of(sums):
            return jnp.concatenate(
                parts_of(sums) + (jnp.zeros_like(sums),), axis=0
            ).astype(BF16)

        near = pl.multiple_of(z * pair, pair)
        early_at = 2 * gvecs - 2 * pair

        def early_background(step):
            @pl.when(step == 0)
            def _():
                @pl.when(c == 0)
                def _():
                    for d in range(1, levels):
                        lead_z_in(d).wait_recv()
                        for q in range(1, col_count):
                            lead_plane(d, q).start()

            @pl.when(step == 2)
            def _():
                @pl.when(c != 0)
                def _():
                    for d in range(1, levels):
                        lead_in(lax.rem(z + d, levels)).wait_recv()

                @pl.when(z >= 1)
                def _():
                    absorb(z - 1)

            @pl.when(step == 3)
            def _():
                @pl.when(z + 1 <= levels - 1)
                def _():
                    absorb(z + 1)

        @pl.loop(0, EARLY)
        def _(step):
            slot = lax.rem(step, 2)
            both, column, masked, stacked = front(step)
            mine = []
            for a in range(2):
                mine.append(rows_sum(jnp.dot(
                    stacked, turned[a, :, pl.ds(near, pair)], preferred_element_type=F32
                )))
            mine.append(smalls(both, masked))
            mine = jnp.concatenate(mine, axis=1)
            outgoing[slot, 0:1, early_at:] = mine
            copies = plane_copies(slot, early_at)
            for copy in copies:
                copy.start()
            early_background(step)
            for copy in copies:
                copy.wait()
            received = message[slot, :, early_at:] + jnp.where(sub1 == c, mine, 0.0)
            sums = received[:, : 2 * pair]
            pieces = pieces_of(sums)
            product = 0.5 * rows_sum(
                jnp.dot(
                    pieces[:, :pair], natural[1, pl.ds(near, pair), :],
                    preferred_element_type=F32,
                )
                + jnp.dot(
                    pieces[:, pair:], natural[0, pl.ds(near, pair), :],
                    preferred_element_type=F32,
                )
            )
            whole_sum = rows_sum(sums)
            square = lanes_sum(whole_sum[:, :pair] * whole_sum[:, pair:])
            small = rows_sum(received[:, 2 * pair :])
            total = zsum(slot, [
                product, partial[pl.ds(step + 2, 1), :], jnp.where(lane1 == 0, square, 0.0),
            ])
            panel[pl.ds(step + 2, 1), :] = total[:, wide : 2 * wide]
            square = lanes_sum(total[:, 2 * wide :])
            settle(step, both, column, total[:, :wide], square, small)

        for o in range(1, levels - 1):
            @pl.when(z - 1 - o >= 0)
            def _():
                absorb(z - 1 - o)

            @pl.when(z + 1 + o <= levels - 1)
            def _():
                absorb(z + 1 + o)

        start = lead_product(0)
        for level in range(1, levels):
            start = start + lead_product(level)
        panel[...] = start

        rows_at = EARLY + 4
        work_at = rows_at + 1

        def background(step):
            @pl.when(step == rows_at)
            def _():
                for level in range(levels):
                    for kk in range(2):
                        row_give(level, kk).wait_recv()

            @pl.when(jnp.logical_and(step >= work_at, step < work_at + row_tiles))
            def _():
                block_work(step - work_at, 1)

        @pl.loop(EARLY, PB)
        def _(step):
            slot = lax.rem(step, 2)
            both, column, masked, stacked = front(step)
            mine = []
            for a in range(2):
                mine.append(
                    rows_sum(jnp.dot(stacked, turned[a], preferred_element_type=F32))
                )
            mine.append(smalls(both, masked))
            mine = jnp.concatenate(mine, axis=1)
            outgoing[slot, 0:1, :] = mine
            copies = plane_copies(slot, 0)
            for copy in copies:
                copy.start()
            background(step)
            for copy in copies:
                copy.wait()
            received = message[slot] + jnp.where(sub1 == c, mine, 0.0)
            sums = received[:, : 2 * gvecs]
            pieces = pieces_of(sums)
            product = 0.5 * rows_sum(
                jnp.dot(pieces[:, :gvecs], natural[1], preferred_element_type=F32)
                + jnp.dot(pieces[:, gvecs:], natural[0], preferred_element_type=F32)
            )
            whole_sum = rows_sum(sums)
            square = lanes_sum(whole_sum[:, :gvecs] * whole_sum[:, gvecs:])
            settle(step, both, column, product, square, rows_sum(received[:, 2 * gvecs :]))

        for side in range(2):
            right[side] = vw[:, side * half : (side + 1) * half]

        def left_out(kc, q):
            return remote(
                right.at[source_half(kc)], left, end_send.at[kc, q], end_recv.at[0],
                (2 * z + kc, q),
            )

        def each_left(action):
            for kc in range(2):
                for q in range(col_count):
                    away = c == source_c(kc)
                    if kc == 1:
                        away = jnp.logical_and(away, c != q)

                    @pl.when(away)
                    def _():
                        action(left_out(kc, q))

        each_left(lambda copy: copy.start())
        right_copy().start()
        ends_copy().start()

        @pl.when(c == source_c(1))
        def _():
            left[...] = right[source_half(1)]

        @pl.when(c != source_c(1))
        def _():
            left_in().wait_recv()

        each_left(lambda copy: copy.wait_send())
        right_copy().wait_send()
        ends_copy().wait_send()
        spin_give().wait_recv()
        eig_copy().wait_send()
        for d in range(col_count):
            across(z, 1, d).wait_send()

        @pl.when(c == 0)
        def _():
            for d in range(levels):
                for q in range(1, col_count):
                    lead_plane(d, q).wait_send()
            for d in range(1, levels):
                lead_z(d).wait_send()

    for d in range(1, col_count):
        first(d).start()

    @pl.when(k == 0)
    def _():
        helper_core()

    @pl.when(is_main)
    def _():
        main_core()

    for d in range(1, col_count):
        first(d).wait_send()


def step(psi, hpsi, eig, sizes):
    row_count, col_count, row_tiles, col_tiles, tile = sizes
    g_rows = psi.shape[0]
    half = row_tiles * tile
    full = col_tiles * tile
    wide = full + tile
    levels = row_count // 2
    gvecs = row_count * col_count * g_rows
    deep = gvecs // row_count
    whole = pl.BlockSpec(memory_space=pltpu.VMEM)
    dma = pltpu.SemaphoreType.DMA

    def both(*shape):
        return [dma(shape), dma(shape)]

    scratch = [
        pltpu.VMEM((g_rows, psi.shape[1]), BF16),
        pltpu.VMEM((g_rows, psi.shape[1]), BF16),
        pltpu.VMEM((2, levels, 2, col_count, g_rows, full), BF16),
        pltpu.VMEM((2, 2, levels, 2, col_count, g_rows, half), BF16),
        pltpu.VMEM((levels, 2, 2, LEAD, deep), BF16),
        pltpu.VMEM((col_count, 2, g_rows, full), BF16),
        pltpu.VMEM((2, gvecs, wide), BF16),
        pltpu.VMEM((2, full, gvecs), BF16),
        pltpu.VMEM((LEAD, wide), F32),
        pltpu.VMEM((LEAD, wide), F32),
        pltpu.VMEM((2 * PB, wide), F32),
        pltpu.VMEM((2, 8, 2 * gvecs + tile), F32),
        pltpu.VMEM((2, 8, 2 * gvecs + tile), F32),
        pltpu.VMEM((3, 8, 2 * wide + tile), F32),
        pltpu.VMEM((3, 8, 2 * wide + tile), F32),
        pltpu.VMEM((2, half, col_tiles, tile), BF16),
        pltpu.VMEM((2, half, full), BF16),
        pltpu.VMEM((levels, 2 * deep, full), F32),
        pltpu.VMEM((levels + 1, 2 * deep, full), F32),
        pltpu.VMEM((deep, col_tiles, tile), F32),
        pltpu.VMEM((deep, col_tiles, tile), BF16),
        *both(col_count),
        *both(levels, 2, col_count), *both(levels, 2, col_count),
        *both(levels, 2, col_count),
        *both(levels),
        dma((levels, col_count)), dma((levels,)),
        dma((2, levels, 2, 2, col_count // 2)), dma((2, levels, 2, 2)),
        dma((2, levels, 2)),
        *both(levels, 2),
        *both(2, col_count), *both(3, levels),
        dma((3, col_count)), dma((3,)),
        *both(1), *both(levels), *both(levels), dma((2,)),
        *both(1),
    ]
    held = sum(
        math.prod(item.shape) * jnp.dtype(item.dtype).itemsize
        for item in scratch if item.memory_space == pltpu.VMEM
    )
    return pl.pallas_call(
        functools.partial(step_kernel, sizes),
        out_shape=(
            jax.ShapeDtypeStruct((half, full), F32),
            jax.ShapeDtypeStruct((half, col_tiles, tile), F32),
            jax.ShapeDtypeStruct((2 * PB, half), F32),
            jax.ShapeDtypeStruct((2, 2 * PB, half), F32),
            jax.ShapeDtypeStruct((8, tile), F32),
            jax.ShapeDtypeStruct((deep, col_tiles, tile), BF16),
        ),
        in_specs=[pl.BlockSpec(memory_space=pltpu.HBM)] * 3,
        out_specs=(whole,) * 6,
        scratch_shapes=scratch,
        compiler_params=pltpu.CompilerParams(
            collective_id=0, has_side_effects=True, vmem_limit_bytes=held + 4 * half * full + 4 * 1024 * 1024
        ),
        cost_estimate=pl.CostEstimate(
            flops=400_000_000, bytes_accessed=4_000_000, transcendentals=0
        ),
        name="step",
    )(psi, hpsi, eig)


def finish_kernel(
    sizes, reduced, correlation, left, right, ends, rotated,
    updated_out, corr_out, diag_out, off_out, rotated_out, updated, sems,
):
    row_count, col_count, row_tiles, col_tiles, tile = sizes

    def place(position):
        return 2 * (position % row_tiles) + position // row_tiles

    spin = pltpu.make_async_copy(rotated, rotated_out, sems.at[0])
    spin.start()
    diag_out[...] = ends[0:1, :PB]
    off_out[...] = ends[1:2, :PB]
    first = pltpu.make_async_copy(correlation, corr_out, sems.at[1])
    first.start()
    moves = [spin, first]
    high, middle, low = parts_of(left[...])
    lhs = jnp.concatenate([high, high, middle, middle, high, low], axis=0).astype(BF16)
    sides = []
    for side in range(2):
        other = right[side]
        other = jnp.concatenate([other[PB:], other[:PB]], axis=0)
        high, middle, low = parts_of(other)
        sides.append(
            jnp.concatenate([high, middle, high, middle, low, high], axis=0).astype(BF16)
        )
    width = row_tiles * tile
    for block in range(row_tiles):
        at = block * tile
        for side in range(2):
            value = reduced[at : at + tile, side * width : (side + 1) * width] - inner(
                lhs[:, at : at + tile], sides[side]
            )
            for t in range(row_tiles):
                updated[at : at + tile, place(side * row_tiles + t), :] = (
                    value[:, t * tile : (t + 1) * tile]
                )
        move = pltpu.make_async_copy(
            updated.at[at : at + tile], updated_out.at[at : at + tile], sems.at[2 + block]
        )
        move.start()
        moves.append(move)
    for move in moves:
        move.wait()


def finish(parts, sizes):
    row_count, col_count, row_tiles, col_tiles, tile = sizes
    whole = pl.BlockSpec(memory_space=pltpu.VMEM)
    hbm = pl.BlockSpec(memory_space=pl.ANY)
    shape = (row_tiles * tile, col_tiles, tile)
    return pl.pallas_call(
        functools.partial(finish_kernel, sizes),
        out_shape=(
            jax.ShapeDtypeStruct(shape, F32), jax.ShapeDtypeStruct(shape, F32),
            jax.ShapeDtypeStruct((1, PB), F32), jax.ShapeDtypeStruct((1, PB), F32),
            jax.ShapeDtypeStruct(parts[-1].shape, BF16),
        ),
        in_specs=[whole] * 6,
        out_specs=(hbm, hbm, whole, whole, hbm),
        scratch_shapes=[
            pltpu.VMEM(shape, F32),
            pltpu.SemaphoreType.DMA((2 + row_tiles,)),
        ],
        compiler_params=pltpu.CompilerParams(vmem_limit_bytes=16 * 1024 * 1024),
        cost_estimate=pl.CostEstimate(
            flops=200_000_000, bytes_accessed=8_000_000, transcendentals=0
        ),
        name="finish",
    )(*parts)


def on_device(psi, hpsi, eigvec):
    row_tiles = eigvec.shape[0]
    tile = eigvec.shape[2]
    col_tiles = eigvec.shape[3]
    row_count = lax.axis_size("row")
    col_count = lax.axis_size("col")
    sizes = (row_count, col_count, row_tiles, col_tiles, tile)
    flat = eigvec.reshape(row_tiles * tile, col_tiles, tile)
    parts = step(psi, hpsi, flat, sizes)
    updated, correlation, diagonal, offdiag, rotated = finish(parts, sizes)
    tile_shape = (row_tiles, 1, tile, col_tiles, 1, tile)
    return (
        correlation.reshape(tile_shape),
        updated.reshape(tile_shape),
        diagonal.reshape(PB),
        offdiag.reshape(PB),
        rotated.reshape(rotated.shape[0], col_tiles, 1, tile),
    )


def solution(mesh):
    return jax.shard_map(
        on_device,
        mesh=mesh,
        in_specs=(
            P(("row", "col"), None),
            P(("row", "col"), None),
            P(None, "row", None, None, "col", None),
        ),
        out_specs=(
            P(None, "row", None, None, "col", None),
            P(None, "row", None, None, "col", None),
            P(),
            P(),
            P("row", None, "col", None),
        ),
        check_vma=False,
    )
```

```python
import functools
import math

import jax
import jax.numpy as jnp
from jax import lax
from jax.experimental import pallas as pl
from jax.experimental.pallas import tpu as pltpu
from jax.sharding import PartitionSpec as P

PB = 16
LEAD = 32
LEAD_ROWS = 24
F32 = jnp.float32
BF16 = jnp.bfloat16
MESH = pl.DeviceIdType.MESH


def inner(left, right):
    return lax.dot_general(
        left, right, (((0,), (0,)), ((), ())), preferred_element_type=F32
    )


def remote(source, target, send, recv, device):
    return pltpu.make_async_remote_copy(
        src_ref=source, dst_ref=target, send_sem=send, recv_sem=recv,
        device_id=device, device_id_type=MESH,
    )


def lanes_sum(array):
    return jnp.sum(array, axis=1, keepdims=True)


def rows_sum(array):
    return jnp.sum(array, axis=0, keepdims=True)


def parts_of(array):
    high = array.astype(BF16).astype(F32)
    rest = array - high
    middle = rest.astype(BF16).astype(F32)
    return high, middle, rest - middle


EARLY = 4


def step_kernel(
    sizes, psi_in, hpsi_in, eig,
    reduced_out, ordered_out, left, right, ends, rotated,
    reduced, ordered, psi, hpsi, col_all, row_all, lead_all, stage, natural, turned, panel, partial, vw,
    message, outgoing, zmessage, zoutgoing, lead_rows, eig_raw, eig_flat, keep, inbox, spun, spun_other,
    s1_send, s1_recv, up_send, up_recv, down_send, down_recv, sib_send, sib_recv,
    leadz_send, leadz_recv, leadp_send, leadp_recv, row_send, row_recv, own_sem,
    give_send, give_recv, msg_send, msg_recv, zmsg_send, zmsg_recv,
    end_send, end_recv, eig_send, eig_recv, upsum_send, upsum_recv, downsum_send, downsum_recv, load_sem, leave_sem,
    spin_send, spin_recv,
):
    row_count, col_count, row_tiles, col_tiles, tile = sizes
    levels = row_count // 2
    half = row_tiles * tile
    full = 2 * half
    wide = full + tile
    gvecs = natural.shape[1]
    deep = gvecs // row_count
    pair = 2 * deep
    r = lax.axis_index("row")
    c = lax.axis_index("col")
    z = lax.div(r, 2)
    k = lax.rem(r, 2)
    is_main = k == 1
    sib = (r + 1 - 2 * k, c)
    partner = c + 1 - 2 * lax.rem(c, 2)
    group = 2 * col_count
    flat_id = k * col_count + c

    def peer(d):
        q = lax.rem(flat_id + d, group)
        return (2 * z + lax.div(q, col_count), lax.rem(q, col_count))

    def along(d):
        return (lax.rem(r + 2 * d, row_count), c)

    def turn(d):
        return lax.rem((partner if d % 2 else c) + 2 * (d // 2), col_count)

    def back(d):
        return d if d < 2 else col_count - d + 2 * (d % 2)

    order = [0] + [back(d) for d in range(1, col_count)]

    loads = [
        pltpu.make_async_copy(psi_in, psi, load_sem.at[0]),
        pltpu.make_async_copy(hpsi_in, hpsi, load_sem.at[1]),
    ]
    for load in loads:
        load.start()
    message[...] = jnp.zeros_like(message)
    zmessage[...] = jnp.zeros_like(zmessage)
    neighbours = [peer(d) for d in range(1, group)] + [along(d) for d in range(1, levels)]
    barrier = pltpu.get_barrier_semaphore()
    for device in neighbours:
        pl.semaphore_signal(barrier, inc=1, device_id=device, device_id_type=MESH)
    for load in loads:
        load.wait()
    for target in range(col_count):
        for a, source in enumerate((psi, hpsi)):
            for parity in range(2):
                for t in range(row_tiles):
                    j = target + col_count * parity + row_count * t
                    at = (parity * row_tiles + t) * tile
                    stage[target, a, :, at : at + tile] = source[:, j * tile : (j + 1) * tile]
    col_all[:, z, k, c] = stage[c]
    pl.semaphore_wait(barrier, len(neighbours))

    def first(d):
        return remote(
            stage.at[turn(d)], col_all.at[:, z, k, c], s1_send.at[d], s1_recv.at[d], (r, turn(d))
        )

    def first_in(d):
        place = col_all.at[:, z, k, turn(back(d))]
        return remote(place, place, s1_send.at[d], s1_recv.at[d], (r, turn(d)))

    def across(level, kk, d):
        place = col_all.at[:, level, kk, turn(d)]
        return remote(
            place, place, sib_send.at[level, kk, d], sib_recv.at[level, kk, d], sib
        )

    def eig_copy():
        return remote(eig, eig_raw.at[1], eig_send.at[0], eig_recv.at[0], sib)

    def row_give(level, kk):
        place = row_all.at[1, :, level, kk]
        return remote(place, place, give_send.at[level, kk], give_recv.at[level, kk], sib)

    def spin_give():
        return remote(spun_other, rotated, spin_send.at[0], spin_recv.at[0], sib)

    def source_c(kc):
        return lax.rem(2 * z + kc, col_count)

    def source_half(kc):
        return lax.div(2 * z + kc, col_count)

    def block_work(index, kc):
        at = pl.multiple_of(index * tile, tile)

        def rows_of(a):
            return row_all[kc, a, :, :, :, :, pl.ds(at, tile)].reshape(gvecs, tile)

        for side in range(2):
            def cols_of(a):
                return col_all[a, :, :, :, :, side * half : (side + 1) * half].reshape(
                    gvecs, half
                )

            result = inner(rows_of(0), cols_of(0)) * (1.0 / gvecs)
            for t in range(row_tiles):
                ordered[pl.ds(at, tile), 2 * t + side, :] = result[:, t * tile : (t + 1) * tile]
            reduced[pl.ds(at, tile), side * half : (side + 1) * half] = 0.5 * (
                inner(rows_of(0), cols_of(1)) + inner(rows_of(1), cols_of(0))
            )

    def leave():
        return [
            pltpu.make_async_copy(reduced, reduced_out, leave_sem.at[0]),
            pltpu.make_async_copy(ordered, ordered_out, leave_sem.at[1]),
        ]

    def helper_core():
        not_top = z < levels - 1
        not_bottom = z > 0

        def up(o, kk, d):
            place = col_all.at[:, z - o, kk, turn(d)]
            return remote(place, place, up_send.at[o, kk, d], up_recv.at[o, kk, d], (r + 2, c))

        def up_in(o, kk, d):
            place = col_all.at[:, z - 1 - o, kk, turn(d)]
            return remote(place, place, up_send.at[o, kk, d], up_recv.at[o, kk, d], (r + 2, c))

        def down(o, kk, d):
            place = col_all.at[:, z + o, kk, turn(d)]
            return remote(
                place, place, down_send.at[o, kk, d], down_recv.at[o, kk, d], (r - 2, c)
            )

        def down_in(o, kk, d):
            place = col_all.at[:, z + 1 + o, kk, turn(d)]
            return remote(
                place, place, down_send.at[o, kk, d], down_recv.at[o, kk, d], (r - 2, c)
            )

        def launch(kk, d):
            @pl.when(not_top)
            def _():
                up(0, kk, d).start()

            @pl.when(not_bottom)
            def _():
                down(0, kk, d).start()

        fan = col_count // 2

        def is_source(kc):
            return c == source_c(kc)

        def is_relay(kc):
            return jnp.logical_and(
                c != source_c(kc), lax.rem(c, 2) == lax.rem(source_c(kc), 2)
            )

        def row_from(kc, level, kk):
            lane0 = pl.multiple_of(source_half(kc) * half, half)
            return col_all.at[:, level, kk, :, :, pl.ds(lane0, half)]

        def row_own(kc, level, kk):
            return pltpu.make_async_copy(
                row_from(kc, level, kk), row_all.at[kc, :, level, kk], own_sem.at[kc, level, kk]
            )

        def row_part(kc, level, kk, a):
            lane0 = pl.multiple_of(source_half(kc) * half, half)
            return col_all.at[a, level, kk, :, :, pl.ds(lane0, half)]

        def row_out(kc, level, kk, a, i):
            device = (r, partner) if i == 0 else (r, lax.rem(c + 2 * i, col_count))
            return remote(
                row_part(kc, level, kk, a), row_all.at[kc, a, level, kk],
                row_send.at[kc, level, kk, a, i], row_recv.at[kc, level, kk, a], device,
            )

        def row_relay(kc, level, kk, a):
            place = row_all.at[kc, a, level, kk]
            return remote(
                place, place, row_send.at[kc, level, kk, a, 0],
                row_recv.at[kc, level, kk, a], (r, partner),
            )

        def row_launch(level):
            for kc in range(2):
                @pl.when(is_source(kc))
                def _():
                    for a in range(2):
                        for kk in range(2):
                            for i in range(fan):
                                row_out(kc, level, kk, a, i).start()
                    for kk in range(2):
                        row_own(kc, level, kk).start()

        def row_finish(level):
            for a in range(2):
                for kk in range(2):
                    for kc in range(2):
                        @pl.when(is_relay(kc))
                        def _():
                            row_relay(kc, level, kk, a).wait_recv()
                            row_relay(kc, level, kk, a).start()

        for d in order:
            if d != 0:
                first_in(back(d)).wait_recv()
            launch(0, d)
            across(z, 0, d).start()
            across(z, 1, d).wait_recv()
            launch(1, d)
        row_launch(z)
        own_eig = pltpu.make_async_copy(eig, eig_raw.at[0], load_sem.at[0])
        own_eig.start()
        own_eig.wait()
        eig_copy().wait_recv()
        for kc in range(2):
            values = eig_raw[kc].astype(F32)
            for g in range(col_tiles):
                eig_flat[kc, :, g * tile : (g + 1) * tile] = values[:, g, :].astype(BF16)
        for o in range(levels - 1):
            below = z - 1 - o >= 0
            above = z + 1 + o <= levels - 1
            for d in order:
                for kk in range(2):
                    @pl.when(below)
                    def _():
                        up_in(o, kk, d).wait_recv()

                        @pl.when(not_top)
                        def _():
                            up(o + 1, kk, d).start()

                        across(z - 1 - o, kk, d).start()

                    @pl.when(above)
                    def _():
                        down_in(o, kk, d).wait_recv()

                        @pl.when(not_bottom)
                        def _():
                            down(o + 1, kk, d).start()

                        across(z + 1 + o, kk, d).start()

            @pl.when(below)
            def _():
                row_launch(z - 1 - o)

            @pl.when(above)
            def _():
                row_launch(z + 1 + o)

            if o == 0:
                row_finish(z)
            else:
                @pl.when(z - o >= 0)
                def _():
                    row_finish(z - o)

                @pl.when(z + o <= levels - 1)
                def _():
                    row_finish(z + o)

        @pl.when(z - (levels - 1) >= 0)
        def _():
            row_finish(z - (levels - 1))

        @pl.when(z + levels - 1 <= levels - 1)
        def _():
            row_finish(z + levels - 1)

        def row_wait(a):
            for level in range(levels):
                for kk in range(2):
                    for kc in range(2):
                        @pl.when(jnp.logical_not(jnp.logical_or(is_source(kc), is_relay(kc))))
                        def _():
                            row_relay(kc, level, kk, a).wait_recv()

        for level in range(levels):
            for kk in range(2):
                for kc in range(2):
                    @pl.when(is_source(kc))
                    def _():
                        row_own(kc, level, kk).wait()

        row_wait(0)

        def upsum(level):
            return remote(
                keep.at[level], inbox.at[level], upsum_send.at[level], upsum_recv.at[level],
                (r + 2, c),
            )

        def downsum(level, place):
            return remote(
                keep.at[level], inbox.at[place], downsum_send.at[level],
                downsum_recv.at[level], (r - 2, c),
            )

        def partial_sum(level):
            keep[level] = jnp.dot(
                row_all[0, 0, level].reshape(pair, half), eig_flat[0],
                preferred_element_type=F32,
            ) + jnp.dot(
                row_all[1, 0, level].reshape(pair, half), eig_flat[1],
                preferred_element_type=F32,
            )

        def send_down(level):
            @pl.when(z - 1 == level)
            def _():
                downsum(level, levels).start()

            @pl.when(z - 1 != level)
            def _():
                downsum(level, level).start()

        for i in range(levels - 1):
            high, low = levels - 1 - i, i

            @pl.when(z < high)
            def _():
                partial_sum(high)

                @pl.when(z == 0)
                def _():
                    upsum(high).start()

            @pl.when(z > low)
            def _():
                partial_sum(low)

                @pl.when(z == levels - 1)
                def _():
                    send_down(low)

        partial_sum(z)
        row_wait(1)
        for level in range(levels):
            for kk in range(2):
                row_give(level, kk).start()

        @pl.loop(0, row_tiles)
        def _(index):
            block_work(index, 0)

        for copy in leave():
            copy.start()

        def pass_up(high):
            @pl.when(jnp.logical_and(z > 0, z < high))
            def _():
                upsum(high).wait_recv()
                keep[high] = keep[high] + inbox[high]
                upsum(high).start()

        def pass_down(low):
            @pl.when(jnp.logical_and(z < levels - 1, z > low))
            def _():
                downsum(low, low).wait_recv()
                keep[low] = keep[low] + inbox[low]
                send_down(low)

        @pl.when(z < levels // 2)
        def _():
            for i in range(levels - 1):
                pass_up(levels - 1 - i)
                pass_down(i)

        @pl.when(z >= levels // 2)
        def _():
            for i in range(levels - 1):
                pass_down(i)
                pass_up(levels - 1 - i)

        @pl.when(z > 0)
        def _():
            upsum(z).wait_recv()
            keep[z] = keep[z] + inbox[z]

        @pl.when(z < levels - 1)
        def _():
            downsum(z, levels).wait_recv()
            keep[z] = keep[z] + inbox[levels]

        for kk in (1, 0):
            for g in range(col_tiles):
                spun[:, g, :] = keep[z, kk * deep : (kk + 1) * deep, g * tile : (g + 1) * tile]
            if kk:
                spun_other[...] = spun[...].astype(BF16)
                spin_give().start()
            else:
                rotated[...] = spun[...].astype(BF16)

        for level in range(levels):
            for kk in range(2):
                for kc in range(2):
                    for a in range(2):
                        @pl.when(is_source(kc))
                        def _():
                            for i in range(fan):
                                row_out(kc, level, kk, a, i).wait_send()

                        @pl.when(is_relay(kc))
                        def _():
                            row_relay(kc, level, kk, a).wait_send()

                row_give(level, kk).wait_send()
                for d in range(col_count):
                    @pl.when(jnp.logical_or(level != z, kk == 0))
                    def _():
                        across(level, kk, d).wait_send()

        for o in range(levels):
            for kk in range(2):
                for d in range(col_count):
                    @pl.when(jnp.logical_and(not_top, z - o >= 0))
                    def _():
                        up(o, kk, d).wait_send()

                    @pl.when(jnp.logical_and(not_bottom, z + o <= levels - 1))
                    def _():
                        down(o, kk, d).wait_send()

        for level in range(levels):
            @pl.when(z < level)
            def _():
                upsum(level).wait_send()

            @pl.when(z > level)
            def _():
                downsum(level, level).wait_send()

        spin_give().wait_send()
        for copy in leave():
            copy.wait()
        left_in().wait_recv()
        right_copy().wait_recv()
        ends_copy().wait_recv()

    def left_in():
        return remote(right.at[0], left, end_send.at[0, 0], end_recv.at[0], (r, c))

    def right_copy():
        return remote(right, right, end_send.at[2, 0], end_recv.at[1], sib)

    def ends_copy():
        return remote(ends, ends, end_send.at[2, 1], end_recv.at[2], sib)

    def main_core():
        for d in order:
            if d != 0:
                first_in(back(d)).wait_recv()
            across(z, 1, d).start()
        eig_copy().start()
        for d in order:
            across(z, 0, d).wait_recv()

        def lead_z(d):
            place = lead_all.at[z]
            return remote(place, place, leadz_send.at[d], leadz_recv.at[d], along(d))

        def lead_z_in(d):
            place = lead_all.at[lax.rem(z + levels - d, levels)]
            return remote(place, place, leadz_send.at[d], leadz_recv.at[d], along(d))

        def lead_plane(d, q):
            level = lax.rem(z + levels - d, levels)
            place = lead_all.at[level]
            return remote(place, place, leadp_send.at[d, q], leadp_recv.at[level], (r, q))

        def lead_in(level):
            place = lead_all.at[level]
            return remote(place, place, leadp_send.at[0, 0], leadp_recv.at[level], (r, c))

        @pl.when(c == 0)
        def _():
            for kk in range(2):
                for a in range(2):
                    block = col_all[a, z, kk, :, :, 0:tile].astype(F32).reshape(deep, tile)
                    lead_all[z, kk, a] = jnp.transpose(block)[0:LEAD].astype(BF16)
            for q in range(1, col_count):
                lead_plane(0, q).start()
            for d in range(1, levels):
                lead_z(d).start()

        def absorb_own(level):
            for kk in range(2):
                at = pl.multiple_of((level * 2 + kk) * deep, deep)
                for a in range(2):
                    own = col_all[a, level, kk].reshape(deep, full)
                    natural[a, pl.ds(at, deep), 0:full] = own
                    turned[a, :, pl.ds(at, deep)] = jnp.transpose(own.astype(F32)).astype(BF16)

        def absorb_lead(level):
            for kk in range(2):
                at = pl.multiple_of((level * 2 + kk) * deep, deep)
                for a in range(2):
                    lead = lead_all[level, kk, a].astype(F32)
                    lead = jnp.concatenate(
                        [lead, jnp.zeros((tile - LEAD, deep), F32)], axis=0
                    )
                    natural[a, pl.ds(at, deep), full:wide] = jnp.transpose(lead).astype(BF16)

        def absorb(level):
            for kk in range(2):
                for d in range(col_count):
                    across(level, kk, d).wait_recv()
            absorb_own(level)
            absorb_lead(level)

        def lead_product(level):
            total = jnp.zeros((LEAD, wide), F32)
            for kk in range(2):
                at = pl.multiple_of((level * 2 + kk) * deep, deep)
                for a in range(2):
                    total = total + jnp.dot(
                        lead_all[level, kk, a], natural[1 - a, pl.ds(at, deep), :],
                        preferred_element_type=F32,
                    )
            return 0.5 * total

        absorb_own(z)

        @pl.when(c != 0)
        def _():
            lead_in(z).wait_recv()

        absorb_lead(z)
        partial[...] = lead_product(z)
        vw[...] = jnp.zeros_like(vw)
        ends[...] = jnp.zeros_like(ends)

        lane = lax.broadcasted_iota(jnp.int32, (1, wide), 1)
        own_tile = lax.div(lane, tile)
        inside = lane - own_tile * tile
        parity = lax.div(own_tile, row_tiles)
        band = c + col_count * parity + row_count * (own_tile - row_tiles * parity)
        pos = jnp.where(lane < full, band * tile + inside, lane - full)
        lane1 = lax.broadcasted_iota(jnp.int32, (1, tile), 1)
        lane2 = lax.broadcasted_iota(jnp.int32, (2 * PB, tile), 1)
        sub2 = lax.broadcasted_iota(jnp.int32, (2 * PB, tile), 0)
        sub8 = lax.broadcasted_iota(jnp.int32, (8, full), 0)
        sub1 = lax.broadcasted_iota(jnp.int32, (8, 1), 0)
        zwidth = 2 * wide + tile

        def swap(column):
            return jnp.concatenate([column[PB:], column[:PB]], axis=0)

        def zcopies(slot):
            return [
                remote(
                    zoutgoing.at[slot, pl.ds(0, 1)], zmessage.at[slot, pl.ds(z, 1)],
                    zmsg_send.at[slot, d], zmsg_recv.at[slot, d], along(d),
                )
                for d in range(1, levels)
            ]

        def zsum(slot, pieces):
            mine = jnp.concatenate(pieces, axis=1)
            zoutgoing[slot, 0:1, :] = mine
            copies = zcopies(slot)
            for copy in copies:
                copy.start()
            for copy in copies:
                copy.wait()
            return rows_sum(zmessage[slot] + jnp.where(sub1 == z, mine, 0.0))

        opening = zsum(2, [partial[0:1, :], partial[1:2, :], jnp.zeros((1, tile), F32)])
        panel[0:1, :] = opening[:, :wide]
        panel[1:2, :] = opening[:, wide : 2 * wide]

        def front(step):
            both = vw[...]
            lead_vw = both[:, full:]
            head = lanes_sum(jnp.where(lane2 == step, lead_vw, 0.0))
            column = panel[pl.ds(step, 1), :] - rows_sum(both * swap(head))
            masked = jnp.where(pos > step + 1, column, 0.0)[:, :full]
            high, middle, low = parts_of(masked)
            stacked = jnp.where(
                sub8 == 0, high, jnp.where(sub8 == 1, middle, jnp.where(sub8 == 2, low, 0.0))
            ).astype(BF16)
            return both, column, masked, stacked

        def smalls(both, masked):
            onto = lanes_sum(both[:, :full] * masked)
            tail = lanes_sum(masked * masked)
            return rows_sum(jnp.where(lane2 == sub2, onto, 0.0)) + jnp.where(
                lane1 == 2 * PB, tail, 0.0
            )

        def plane_copies(slot, at):
            return [
                remote(
                    outgoing.at[slot, pl.ds(0, 1), at:], message.at[slot, pl.ds(c, 1), at:],
                    msg_send.at[slot, d], msg_recv.at[slot, d],
                    (r, lax.rem(c + d, col_count)),
                )
                for d in range(1, col_count)
            ]

        def settle(step, both, column, product, square, small):
            lead_column = column[:, full:]
            pivot = lanes_sum(jnp.where(lane1 == step + 1, lead_column, 0.0))
            here = lanes_sum(jnp.where(lane1 == step, lead_column, 0.0))
            next_row = panel[pl.ds(step + 1, 1), :]
            corner = lanes_sum(jnp.where(lane1 == step + 1, next_row[:, full:], 0.0))
            head_next = lanes_sum(jnp.where(lane2 == step + 1, both[:, full:], 0.0))
            tail = lanes_sum(jnp.where(lane1 == 2 * PB, small, 0.0))
            onto = lanes_sum(jnp.where(lane2 == sub2, small, 0.0))
            length = jnp.sqrt(pivot * pivot + tail)
            beta = jnp.where(pivot >= 0.0, -length, length)
            tau = (beta - pivot) / beta
            inverse = 1.0 / (pivot - beta)
            vector = jnp.where(
                pos == step + 1, 1.0, jnp.where(pos > step + 1, column * inverse, 0.0)
            )
            onto = onto * inverse + head_next
            image = tau * (product * inverse + next_row - rows_sum(both * swap(onto)))
            edge = lanes_sum(jnp.where(lane1 == step + 1, product[:, full:], 0.0))
            energy = square * inverse * inverse + 2.0 * inverse * edge + corner
            overlap = tau * (energy - 2.0 * rows_sum(onto[:PB] * onto[PB:]))
            image = image - 0.5 * tau * overlap * vector
            vw[pl.ds(step, 1), :] = vector
            vw[pl.ds(PB + step, 1), :] = image
            ends[0:1, :] = jnp.where(lane1 == step, here, ends[0:1, :])
            ends[1:2, :] = jnp.where(lane1 == step, beta, ends[1:2, :])

        def pieces_of(sums):
            return jnp.concatenate(
                parts_of(sums) + (jnp.zeros_like(sums),), axis=0
            ).astype(BF16)

        near = pl.multiple_of(z * pair, pair)
        early_at = 2 * gvecs - 2 * pair

        def early_background(step):
            @pl.when(step == 0)
            def _():
                @pl.when(c == 0)
                def _():
                    for d in range(1, levels):
                        lead_z_in(d).wait_recv()
                        for q in range(1, col_count):
                            lead_plane(d, q).start()

            @pl.when(step == 2)
            def _():
                @pl.when(c != 0)
                def _():
                    for d in range(1, levels):
                        lead_in(lax.rem(z + d, levels)).wait_recv()

                @pl.when(z >= 1)
                def _():
                    absorb(z - 1)

            @pl.when(step == 3)
            def _():
                @pl.when(z + 1 <= levels - 1)
                def _():
                    absorb(z + 1)

        @pl.loop(0, EARLY)
        def _(step):
            slot = lax.rem(step, 2)
            both, column, masked, stacked = front(step)
            mine = []
            for a in range(2):
                mine.append(rows_sum(jnp.dot(
                    stacked, turned[a, :, pl.ds(near, pair)], preferred_element_type=F32
                )))
            mine.append(smalls(both, masked))
            mine = jnp.concatenate(mine, axis=1)
            outgoing[slot, 0:1, early_at:] = mine
            copies = plane_copies(slot, early_at)
            for copy in copies:
                copy.start()
            early_background(step)
            for copy in copies:
                copy.wait()
            received = message[slot, :, early_at:] + jnp.where(sub1 == c, mine, 0.0)
            sums = received[:, : 2 * pair]
            pieces = pieces_of(sums)
            product = 0.5 * rows_sum(
                jnp.dot(
                    pieces[:, :pair], natural[1, pl.ds(near, pair), :],
                    preferred_element_type=F32,
                )
                + jnp.dot(
                    pieces[:, pair:], natural[0, pl.ds(near, pair), :],
                    preferred_element_type=F32,
                )
            )
            whole_sum = rows_sum(sums)
            square = lanes_sum(whole_sum[:, :pair] * whole_sum[:, pair:])
            small = rows_sum(received[:, 2 * pair :])
            total = zsum(slot, [
                product, partial[pl.ds(step + 2, 1), :], jnp.where(lane1 == 0, square, 0.0),
            ])
            panel[pl.ds(step + 2, 1), :] = total[:, wide : 2 * wide]
            square = lanes_sum(total[:, 2 * wide :])
            settle(step, both, column, total[:, :wide], square, small)

        for o in range(1, levels - 1):
            @pl.when(z - 1 - o >= 0)
            def _():
                absorb(z - 1 - o)

            @pl.when(z + 1 + o <= levels - 1)
            def _():
                absorb(z + 1 + o)

        start = lead_product(0)
        for level in range(1, levels):
            start = start + lead_product(level)
        panel[...] = start
        for level in range(levels):
            for kk in range(2):
                for a in range(2):
                    at = a * gvecs + (level * 2 + kk) * deep
                    lead_rows[:, at : at + deep] = (
                        0.5 * lead_all[level, kk, 1 - a].astype(F32)[:LEAD_ROWS]
                    )

        rows_at = EARLY + 3
        work_at = rows_at + 1

        def background(step):
            @pl.when(step == rows_at)
            def _():
                for level in range(levels):
                    for kk in range(2):
                        row_give(level, kk).wait_recv()

            @pl.when(jnp.logical_and(step >= work_at, step < work_at + row_tiles))
            def _():
                block_work(step - work_at, 1)

            @pl.when(step == work_at + row_tiles)
            def _():
                for copy in leave():
                    copy.start()

        @pl.loop(EARLY, PB)
        def _(step):
            slot = lax.rem(step, 2)
            both, column, masked, stacked = front(step)
            mine = []
            for a in range(2):
                mine.append(
                    rows_sum(jnp.dot(stacked, turned[a], preferred_element_type=F32))
                )
            mine.append(smalls(both, masked))
            mine = jnp.concatenate(mine, axis=1)
            outgoing[slot, 0:1, :] = mine
            copies = plane_copies(slot, 0)
            for copy in copies:
                copy.start()
            background(step)
            for copy in copies:
                copy.wait()
            received = message[slot] + jnp.where(sub1 == c, mine, 0.0)
            sums = received[:, : 2 * gvecs]
            pieces = pieces_of(sums)
            product = 0.5 * rows_sum(
                jnp.dot(pieces[:, :gvecs], natural[1, :, :full], preferred_element_type=F32)
                + jnp.dot(pieces[:, gvecs:], natural[0, :, :full], preferred_element_type=F32)
            )
            whole_sum = rows_sum(sums)
            edge_rows = lanes_sum(lead_rows[...] * whole_sum)
            edge_rows = rows_sum(
                jnp.where(lane2[:LEAD_ROWS] == sub2[:LEAD_ROWS], edge_rows, 0.0)
            )
            product = jnp.concatenate([product, edge_rows], axis=1)
            square = lanes_sum(whole_sum[:, :gvecs] * whole_sum[:, gvecs:])
            settle(step, both, column, product, square, rows_sum(received[:, 2 * gvecs :]))

        for side in range(2):
            right[side] = vw[:, side * half : (side + 1) * half]

        def left_out(kc, q):
            return remote(
                right.at[source_half(kc)], left, end_send.at[kc, q], end_recv.at[0],
                (2 * z + kc, q),
            )

        def each_left(action):
            for kc in range(2):
                for q in range(col_count):
                    away = c == source_c(kc)
                    if kc == 1:
                        away = jnp.logical_and(away, c != q)

                    @pl.when(away)
                    def _():
                        action(left_out(kc, q))

        each_left(lambda copy: copy.start())
        right_copy().start()
        ends_copy().start()

        @pl.when(c == source_c(1))
        def _():
            left[...] = right[source_half(1)]

        @pl.when(c != source_c(1))
        def _():
            left_in().wait_recv()

        for copy in leave():
            copy.wait()
        each_left(lambda copy: copy.wait_send())
        right_copy().wait_send()
        ends_copy().wait_send()
        spin_give().wait_recv()
        eig_copy().wait_send()
        for d in range(col_count):
            across(z, 1, d).wait_send()

        @pl.when(c == 0)
        def _():
            for d in range(levels):
                for q in range(1, col_count):
                    lead_plane(d, q).wait_send()
            for d in range(1, levels):
                lead_z(d).wait_send()

    for d in range(1, col_count):
        first(d).start()

    @pl.when(k == 0)
    def _():
        helper_core()

    @pl.when(is_main)
    def _():
        main_core()

    for d in range(1, col_count):
        first(d).wait_send()


def step(psi, hpsi, eig, sizes):
    row_count, col_count, row_tiles, col_tiles, tile = sizes
    g_rows = psi.shape[0]
    half = row_tiles * tile
    full = col_tiles * tile
    wide = full + tile
    levels = row_count // 2
    gvecs = row_count * col_count * g_rows
    deep = gvecs // row_count
    whole = pl.BlockSpec(memory_space=pltpu.VMEM)
    dma = pltpu.SemaphoreType.DMA

    def both(*shape):
        return [dma(shape), dma(shape)]

    scratch = [
        pltpu.VMEM((half, full), F32),
        pltpu.VMEM((half, col_tiles, tile), F32),
        pltpu.VMEM((g_rows, psi.shape[1]), BF16),
        pltpu.VMEM((g_rows, psi.shape[1]), BF16),
        pltpu.VMEM((2, levels, 2, col_count, g_rows, full), BF16),
        pltpu.VMEM((2, 2, levels, 2, col_count, g_rows, half), BF16),
        pltpu.VMEM((levels, 2, 2, LEAD, deep), BF16),
        pltpu.VMEM((col_count, 2, g_rows, full), BF16),
        pltpu.VMEM((2, gvecs, wide), BF16),
        pltpu.VMEM((2, full, gvecs), BF16),
        pltpu.VMEM((LEAD, wide), F32),
        pltpu.VMEM((LEAD, wide), F32),
        pltpu.VMEM((2 * PB, wide), F32),
        pltpu.VMEM((2, 8, 2 * gvecs + tile), F32),
        pltpu.VMEM((2, 8, 2 * gvecs + tile), F32),
        pltpu.VMEM((3, 8, 2 * wide + tile), F32),
        pltpu.VMEM((3, 8, 2 * wide + tile), F32),
        pltpu.VMEM((LEAD_ROWS, 2 * gvecs), F32),
        pltpu.VMEM((2, half, col_tiles, tile), BF16),
        pltpu.VMEM((2, half, full), BF16),
        pltpu.VMEM((levels, 2 * deep, full), F32),
        pltpu.VMEM((levels + 1, 2 * deep, full), F32),
        pltpu.VMEM((deep, col_tiles, tile), F32),
        pltpu.VMEM((deep, col_tiles, tile), BF16),
        *both(col_count),
        *both(levels, 2, col_count), *both(levels, 2, col_count),
        *both(levels, 2, col_count),
        *both(levels),
        dma((levels, col_count)), dma((levels,)),
        dma((2, levels, 2, 2, col_count // 2)), dma((2, levels, 2, 2)),
        dma((2, levels, 2)),
        *both(levels, 2),
        *both(2, col_count), *both(3, levels),
        dma((3, col_count)), dma((3,)),
        *both(1), *both(levels), *both(levels), dma((2,)), dma((2,)),
        *both(1),
    ]
    held = sum(
        math.prod(item.shape) * jnp.dtype(item.dtype).itemsize
        for item in scratch if item.memory_space == pltpu.VMEM
    )
    return pl.pallas_call(
        functools.partial(step_kernel, sizes),
        out_shape=(
            jax.ShapeDtypeStruct((half, full), F32),
            jax.ShapeDtypeStruct((half, col_tiles, tile), F32),
            jax.ShapeDtypeStruct((2 * PB, half), F32),
            jax.ShapeDtypeStruct((2, 2 * PB, half), F32),
            jax.ShapeDtypeStruct((8, tile), F32),
            jax.ShapeDtypeStruct((deep, col_tiles, tile), BF16),
        ),
        in_specs=[pl.BlockSpec(memory_space=pltpu.HBM)] * 3,
        out_specs=(pl.BlockSpec(memory_space=pl.ANY),) * 2 + (whole,) * 4,
        scratch_shapes=scratch,
        compiler_params=pltpu.CompilerParams(
            collective_id=0, has_side_effects=True, vmem_limit_bytes=held + 4 * half * full + 4 * 1024 * 1024
        ),
        cost_estimate=pl.CostEstimate(
            flops=400_000_000, bytes_accessed=4_000_000, transcendentals=0
        ),
        name="step",
    )(psi, hpsi, eig)


def finish_kernel(
    sizes, reduced, correlation, left, right, ends, rotated,
    updated_out, corr_out, diag_out, off_out, rotated_out, updated, sems,
):
    row_count, col_count, row_tiles, col_tiles, tile = sizes

    def place(position):
        return 2 * (position % row_tiles) + position // row_tiles

    spin = pltpu.make_async_copy(rotated, rotated_out, sems.at[0])
    spin.start()
    diag_out[...] = ends[0:1, :PB]
    off_out[...] = ends[1:2, :PB]
    first = pltpu.make_async_copy(correlation, corr_out, sems.at[1])
    first.start()
    moves = [spin, first]
    high, middle, low = parts_of(left[...])
    lhs = jnp.concatenate([high, high, middle, middle, high, low], axis=0).astype(BF16)
    sides = []
    for side in range(2):
        other = right[side]
        other = jnp.concatenate([other[PB:], other[:PB]], axis=0)
        high, middle, low = parts_of(other)
        sides.append(
            jnp.concatenate([high, middle, high, middle, low, high], axis=0).astype(BF16)
        )
    width = row_tiles * tile
    for block in range(row_tiles):
        at = block * tile
        for side in range(2):
            value = reduced[at : at + tile, side * width : (side + 1) * width] - inner(
                lhs[:, at : at + tile], sides[side]
            )
            for t in range(row_tiles):
                updated[at : at + tile, place(side * row_tiles + t), :] = (
                    value[:, t * tile : (t + 1) * tile]
                )
        move = pltpu.make_async_copy(
            updated.at[at : at + tile], updated_out.at[at : at + tile], sems.at[2 + block]
        )
        move.start()
        moves.append(move)
    for move in moves:
        move.wait()


def finish(parts, sizes):
    row_count, col_count, row_tiles, col_tiles, tile = sizes
    whole = pl.BlockSpec(memory_space=pltpu.VMEM)
    hbm = pl.BlockSpec(memory_space=pl.ANY)
    shape = (row_tiles * tile, col_tiles, tile)
    return pl.pallas_call(
        functools.partial(finish_kernel, sizes),
        out_shape=(
            jax.ShapeDtypeStruct(shape, F32), jax.ShapeDtypeStruct(shape, F32),
            jax.ShapeDtypeStruct((1, PB), F32), jax.ShapeDtypeStruct((1, PB), F32),
            jax.ShapeDtypeStruct(parts[-1].shape, BF16),
        ),
        in_specs=[whole, hbm, whole, whole, whole, hbm],
        out_specs=(hbm, hbm, whole, whole, hbm),
        scratch_shapes=[
            pltpu.VMEM(shape, F32),
            pltpu.SemaphoreType.DMA((2 + row_tiles,)),
        ],
        compiler_params=pltpu.CompilerParams(vmem_limit_bytes=16 * 1024 * 1024),
        cost_estimate=pl.CostEstimate(
            flops=200_000_000, bytes_accessed=8_000_000, transcendentals=0
        ),
        name="finish",
    )(*parts)


def on_device(psi, hpsi, eigvec):
    row_tiles = eigvec.shape[0]
    tile = eigvec.shape[2]
    col_tiles = eigvec.shape[3]
    row_count = lax.axis_size("row")
    col_count = lax.axis_size("col")
    sizes = (row_count, col_count, row_tiles, col_tiles, tile)
    flat = eigvec.reshape(row_tiles * tile, col_tiles, tile)
    parts = step(psi, hpsi, flat, sizes)
    updated, correlation, diagonal, offdiag, rotated = finish(parts, sizes)
    tile_shape = (row_tiles, 1, tile, col_tiles, 1, tile)
    return (
        correlation.reshape(tile_shape),
        updated.reshape(tile_shape),
        diagonal.reshape(PB),
        offdiag.reshape(PB),
        rotated.reshape(rotated.shape[0], col_tiles, 1, tile),
    )


def solution(mesh):
    return jax.shard_map(
        on_device,
        mesh=mesh,
        in_specs=(
            P(("row", "col"), None),
            P(("row", "col"), None),
            P(None, "row", None, None, "col", None),
        ),
        out_specs=(
            P(None, "row", None, None, "col", None),
            P(None, "row", None, None, "col", None),
            P(),
            P(),
            P("row", None, "col", None),
        ),
        check_vma=False,
    )
```
